32 devices in a mesh: dp: 4 (over x, core), rows: 8 (over z, y).
Axes of the slice: x: 2, y: 2, z: 4, core: 2. Of those that a mesh axis runs over, the one named last changes fastest.
Arguments:
- grads: bfloat16 [2, 4096, 14336], P(None, 'rows', 'dp'), may hold values from -64 to 64
- basis: bfloat16 [2, 4096, 512], P(None, 'rows'), may hold values from -0.09375 to 0.09375
- moment1: float32 [2, 512, 14336], P(None, 'rows', 'dp'), may hold values from -0.3 to 0.3
- moment2: float32 [2, 512, 14336], P(None, 'rows', 'dp'), may hold values from 0.001 to 0.03
- weights: bfloat16 [2, 4096, 14336], P(None, 'rows', 'dp'), may hold values from -0.09375 to 0.09375
Outputs:
- new_weights: bfloat16 [2, 4096, 14336], P(None, 'rows')
- new_moment1: float32 [2, 512, 14336], P(None, 'rows', 'dp')
- new_moment2: float32 [2, 512, 14336], P(None, 'rows', 'dp')
The draws below stay inside these ranges and needn't reach their ends.
All inputs are finite; a program needn't handle non-finite values.
Results may differ from the reference program's by a relative error of at most 0.00115.
The reference program's roundings to bfloat16 on the way count: a program that leaves them out, or rounds other values in their place, can miss the bound.
Values may be sent and summed in bfloat16 or wider, within the bound.
A program may use at most 128 MiB of HBM per device.

```python
import math
import jax
import jax.numpy as jnp

D = 4096
FF = 14336
RANK = 512
MATS = 2
STEP = 10


def draw_grads(key, part):
    key_rows = jax.random.fold_in(key, 11)
    key_cols = jax.random.fold_in(key, 12)
    primary_key = jax.random.fold_in(key, 13)
    row_scale = jnp.repeat(jnp.exp(jax.random.uniform(key_rows, (MATS, D // 32, 1), jnp.float32, -0.7, 0.7)), 32, axis=1)
    col_scale = jnp.repeat(jnp.exp(jax.random.uniform(key_cols, (MATS, 1, FF // 128), jnp.float32, -0.7, 0.7)), 128, axis=2)
    values = 8.0 * jax.random.normal(primary_key, (MATS, D, FF), jnp.float32) * row_scale * col_scale
    return jnp.clip(values, -64.0, 64.0).astype(jnp.bfloat16)


def block_scale(own_key, shape, cuts, low, high):
    factor_of, own = 1.0, jax.random.fold_in(own_key, 6)
    for dim, parts in cuts:
        heights = jnp.exp(jax.random.uniform(jax.random.fold_in(own, dim), (parts,), jnp.float32, low / len(cuts), high / len(cuts)))
        factor_of = factor_of * jnp.repeat(heights, shape[dim] // parts).reshape([-1 if axis == dim else 1 for axis in range(len(shape))])
    return factor_of


def scatter_about(own_key, dims, deviation, most, cuts=(), held_as=jnp.bfloat16):
    entries = deviation * jax.random.normal(own_key, dims, jnp.float32)
    if cuts:
        entries = entries * block_scale(own_key, dims, cuts, -0.22, 0.18)
    return jnp.clip(entries, -most, most).astype(held_as)


def setup_inputs(seed: int = 0) -> dict:
    keys = jax.random.split(jax.random.key(seed), 6)
    grads = draw_grads(jax.random.fold_in(keys[5], 71), 0)
    basis = scatter_about(keys[1], (MATS, D, RANK), D ** -0.5, 0.09375, ((1, 8),))
    moment1 = scatter_about(keys[2], (MATS, RANK, FF), 0.05, 0.3, ((1, 8), (2, 4)), jnp.float32)
    moment2 = jnp.clip(jnp.exp(math.log(0.03) - 3.4011973 * jax.random.uniform(keys[3], (MATS, RANK, FF), jnp.float32) ** block_scale(keys[3], (MATS, RANK, FF), ((1, 8), (2, 4)), -0.2, 0.2)), 0.001, 0.03)
    weights = scatter_about(keys[4], (MATS, D, FF), D ** -0.5, 0.09375, ((1, 8), (2, 4)))
    return dict(grads=grads, basis=basis, moment1=moment1, moment2=moment2, weights=weights)


def reference(grads, basis, moment1, moment2, weights):
    total = jnp.float32(0.0)
    for index in range(MATS):
        grad_block = grads[index].astype(jnp.float32)
        total = total + jnp.sum(grad_block * grad_block)
    limit = 1.0 * math.sqrt(MATS * D * FF)
    scale = limit / jnp.maximum(jnp.sqrt(total), limit)
    first_bias_correction = 1.0 - 0.9 ** STEP
    second_fix = 1.0 - 0.999 ** STEP
    out_weights = []
    out_first = []
    out_second = []
    for index in range(MATS):
        base = basis[index].astype(jnp.float32)
        projected = jnp.dot(base.T, grads[index].astype(jnp.float32), preferred_element_type=jnp.float32)
        scaled = scale * projected
        first = 0.9 * moment1[index] + 0.1 * scaled
        second = 0.999 * moment2[index] + 0.001 * scaled * scaled
        low_rank_update = (first / first_bias_correction / (jnp.sqrt(second / second_fix) + 1e-08)).astype(jnp.bfloat16)
        projected_back = jnp.dot(base, low_rank_update.astype(jnp.float32), preferred_element_type=jnp.float32)
        out_weights.append((weights[index].astype(jnp.float32) - 0.5 * projected_back).astype(jnp.bfloat16))
        out_first.append(first)
        out_second.append(second)
    return (jnp.stack(out_weights), jnp.stack(out_first), jnp.stack(out_second))
```

```python
import math

import jax
import jax.numpy as jnp
from jax import lax
from jax.experimental import pallas as pl
from jax.experimental.pallas import tpu as pltpu
from jax.sharding import PartitionSpec as P

STEP = 10
SPLITS = 2
LONGEST_RING = 8
CHUNK = 256
VMEM_LIMIT = 60 * 1024 * 1024


def moment_step(projected, moment1, moment2, scale):
    scaled = scale * projected
    first = 0.9 * moment1 + 0.1 * scaled
    second = 0.999 * moment2 + 0.001 * scaled * scaled
    first_bias_correction = 1.0 - 0.9**STEP
    second_fix = 1.0 - 0.999**STEP
    low_rank_update = (
        first / first_bias_correction / (jnp.sqrt(second / second_fix) + 1e-08)
    ).astype(jnp.bfloat16)
    return (first, second, low_rank_update)


def tile_of(width):
    tile = 128
    for cand in range(128, 1025, 128):
        if width % cand == 0:
            tile = cand
    return tile


def place(groups, pieces, out, shape, mat, split):
    count = len(pieces)
    rows, width = pieces[0].shape
    tile = tile_of(width)
    tiles = width // tile

    def piece_spec(p):
        def index(i, j, groups_ref):
            return (0, jnp.where(i == p, j, jnp.where(i < p, 0, tiles - 1)))

        return pl.BlockSpec((rows, tile), index)

    def out_index(i, j, groups_ref):
        return (mat, 0, groups_ref[i] * (SPLITS * tiles) + split * tiles + j)

    def kernel(groups_ref, *refs):
        out_ref = refs[-1]
        for p in range(count):

            @pl.when(pl.program_id(0) == p)
            def _():
                out_ref[0] = refs[p][...]

    extra = [] if out is None else [out]
    return pl.pallas_call(
        kernel,
        grid_spec=pltpu.PrefetchScalarGridSpec(
            num_scalar_prefetch=1,
            grid=(count, tiles),
            in_specs=[piece_spec(p) for p in range(count)]
            + [pl.BlockSpec(memory_space=pl.ANY) for _ in extra],
            out_specs=pl.BlockSpec((1, rows, tile), out_index),
        ),
        out_shape=jax.ShapeDtypeStruct(shape, pieces[0].dtype),
        input_output_aliases={} if out is None else {1 + count: 0},
        cost_estimate=pl.CostEstimate(
            flops=0, bytes_accessed=4 * count * rows * width, transcendentals=0
        ),
        name="place",
    )(groups, *pieces, *extra)


def fused_step(mesh_shape, chunk, grads, basis, moment1, moment2, weights, limit):
    mats, rows, cols = grads.shape
    rank = basis.shape[2]
    height = moment1.shape[1]
    dp = mesh_shape["dp"]
    line = mesh_shape["rows"] // 2
    band = 2 * height
    half = chunk // 2
    per = cols // chunk
    count = mats * per
    hops = line - 1
    ahead = 3
    deep, few = 8, 4
    back_lag = 2 * line
    ticks = count + back_lag + 4
    f32, bf16 = jnp.float32, jnp.bfloat16

    def kernel(
        grads_ref, basis_ref, first_ref, second_ref, weights_ref,
        out, new_first, new_second,
        gv, raw, own_b, pair_b, turned, m1, m2, wv,
        part, rup, rdn, proj, upd, sq_out, sq_in, scale_v,
        raw_s, raw_r, bas_s, bas_r, load, rs_s, rs_r, proj_s, proj_r,
        upd_s, upd_r, ag_s, ag_r, x_s, x_r, core_s, core_r, fwd_s, fwd_r,
        sq_s, sq_r, store, fresh_v, own_s,
    ):
        me, row = lax.axis_index("dp"), lax.axis_index("rows")
        z, y = row // 2, row % 2
        flip = line - 1 - z
        core_peer = me + 1 - 2 * (me % 2)
        x_peer = (me + 2) % dp
        y_peer = row + 1 - 2 * y
        above = jnp.minimum(z + 1, line - 1) * 2 + y
        below = jnp.maximum(z - 1, 0) * 2 + y

        def remote(src, dst, s, r, device):
            return pltpu.make_async_remote_copy(
                src_ref=src, dst_ref=dst, send_sem=s, recv_sem=r,
                device_id=device, device_id_type=pl.DeviceIdType.MESH,
            )

        def rows_at(b):
            return pl.ds(pl.multiple_of(b * band, band), band)

        def spot(c):
            return c // per, c % per

        def cols_at(j):
            return pl.ds(pl.multiple_of(j * chunk, chunk), chunk)

        def out_at(owner, j):
            return pl.ds(pl.multiple_of(owner * cols + j * chunk, 128), chunk)

        def raw_copy(c):
            m, j = spot(c)
            src = pl.ds(pl.multiple_of(j * chunk + (1 - y) * half, half), half)
            dst = pl.ds(pl.multiple_of(j * half, half), half)
            return remote(
                grads_ref.at[m, :, src], raw.at[m, :, dst],
                raw_s.at[c], raw_r.at[c], (me, y_peer),
            )

        def basis_copy(m):
            return remote(
                basis_ref.at[m], pair_b.at[m], bas_s.at[m], bas_r.at[m], (me, y_peer)
            )

        def up_block(t):
            return line - 1 - t + z

        def down_block(t):
            return t - line + 1 + z

        def rs_copy(c, t, way, b):
            slot = c % few
            buf, dev = (rup, above) if way == 0 else (rdn, below)
            return remote(
                part.at[c % deep, rows_at(b), :], buf.at[slot, t],
                rs_s.at[way, slot, t], rs_r.at[way, slot, t], (me, dev),
            )

        def rs_sends(c, t, act):
            @pl.when((z <= line - 2) & (z <= t))
            def _():
                act(rs_copy(c, t, 0, up_block(t)))

            @pl.when((z >= 1) & (flip <= t))
            def _():
                act(rs_copy(c, t, 1, down_block(t)))

        def rs_recv(c, t):
            slot = c % few

            @pl.when((z >= 1) & (z <= t))
            def _():
                rs_copy(c, t - 1, 0, z).wait_recv()
                b = rows_at(up_block(t))
                part[c % deep, b, :] = part[c % deep, b, :] + rup[slot, t - 1]

            @pl.when((flip >= 1) & (flip <= t))
            def _():
                rs_copy(c, t - 1, 1, z).wait_recv()
                b = rows_at(down_block(t))
                part[c % deep, b, :] = part[c % deep, b, :] + rdn[slot, t - 1]

        def proj_copy(c):
            src = pl.ds(pl.multiple_of(z * band + (1 - y) * height, height), height)
            dst = pl.ds(pl.multiple_of(y * half, half), half)
            return remote(
                part.at[c % deep, src, :], proj.at[c % few, :, dst],
                proj_s.at[c % few], proj_r.at[c % few], (me, y_peer),
            )

        def own_rows():
            return pl.ds(pl.multiple_of(row * height, height), height)

        def upd_copy(c):
            ref = upd.at[c % deep, own_rows(), :]
            return remote(ref, ref, upd_s.at[c % few], upd_r.at[c % few], (me, y_peer))

        def ag_copy(c, t, way, b):
            ref = upd.at[c % deep, rows_at(b), :]
            dev = above if way == 0 else below
            return remote(
                ref, ref, ag_s.at[way, c % few, t], ag_r.at[way, c % few, t], (me, dev)
            )

        def ag_sends(c, t, act):
            @pl.when((z <= line - 2) & (z >= t))
            def _():
                act(ag_copy(c, t, 0, z - t))

            @pl.when((z >= 1) & (z + t <= line - 1))
            def _():
                act(ag_copy(c, t, 1, z + t))

        def ag_recv(c, t):
            @pl.when(z >= t + 1)
            def _():
                ag_copy(c, t, 0, z - 1 - t).wait_recv()

            @pl.when(z + 1 + t <= line - 1)
            def _():
                ag_copy(c, t, 1, z + 1 + t).wait_recv()

        def x_copy(c, owner):
            m, j = spot(c)
            ref = out.at[m, :, out_at(owner, j)]
            return remote(fresh_v.at[c % deep], ref, x_s.at[c % deep], x_r.at[c % deep], (x_peer, row))

        def core_copy(c, owner):
            m, j = spot(c)
            ref = out.at[m, :, out_at(owner, j)]
            return remote(
                fresh_v.at[c % deep], ref, core_s.at[c % deep], core_r.at[c % deep], (core_peer, row)
            )

        def own_copy(c):
            m, j = spot(c)
            return pltpu.make_async_copy(
                fresh_v.at[c % deep], out.at[m, :, out_at(me, j)], own_s.at[c % deep]
            )

        def fwd_copy(c, owner):
            m, j = spot(c)
            ref = out.at[m, :, out_at(owner, j)]
            return remote(
                ref, ref, fwd_s.at[c % deep], fwd_r.at[c % deep], (core_peer, row)
            )

        def start(copy):
            copy.start()

        def sent(copy):
            copy.wait_send()

        loads = [
            pltpu.make_async_copy(basis_ref, own_b, load.at[0]),
            pltpu.make_async_copy(first_ref, m1, load.at[1]),
            pltpu.make_async_copy(second_ref, m2, load.at[2]),
            pltpu.make_async_copy(weights_ref, wv, load.at[3]),
        ]
        grad_loads = [
            pltpu.make_async_copy(grads_ref.at[m], gv.at[m], load.at[4 + m])
            for m in range(mats)
        ]
        loads[0].start()
        for copy in grad_loads:
            copy.start()
        for copy in loads[1:]:
            copy.start()

        barrier = pltpu.get_barrier_semaphore()
        peers = [(core_peer, row), (x_peer, row), (me, y_peer)] + [
            (me, ((z + d) % line) * 2 + y) for d in range(1, line)
        ]
        for device in peers:
            pl.semaphore_signal(
                barrier, inc=1, device_id=device, device_id_type=pl.DeviceIdType.MESH
            )
        pl.semaphore_wait(barrier, len(peers))

        raw_copy(0).start()
        basis_copy(0).start()
        for c in range(1, ahead):
            raw_copy(c).start()

        def turn(which, ref, m):
            for i in range(0, rows, 128):
                turned[which, m, :, i : i + 128] = ref[m, i : i + 128, :].T

        loads[0].wait()
        for m in range(mats):
            turn(0, own_b, m)

        squares = jnp.zeros((16, 128), f32)
        for m in range(mats):
            grad_loads[m].wait()

            def square(i, acc, m=m):
                wide = gv[m, pl.ds(pl.multiple_of(i * 16, 16), 16), :].astype(f32)
                wide = wide * wide
                for k in range(0, cols, 128):
                    acc = acc + wide[:, k : k + 128]
                return acc

            squares = lax.fori_loop(0, rows // 16, square, squares)
        sq_out[0] = squares[:8] + squares[8:]

        def sq_copy(k, device, slot):
            return remote(sq_out.at[k], sq_in.at[slot], sq_s.at[slot], sq_r.at[slot], device)

        def sq_line(d):
            return sq_copy(3, (me, ((z + d) % line) * 2 + y), 2 + d)

        sq_copy(0, (core_peer, row), 0).start()
        for copy in loads[1:]:
            copy.wait()
        basis_copy(0).wait_recv()
        turn(1, pair_b, 0)

        def tick(now, carry):
            def stage(lag, body):
                c = now - lag

                @pl.when((c >= 0) & (c < count))
                def _():
                    body(c)

            @pl.when(now + ahead < count)
            def _():
                raw_copy(now + ahead).start()

            for m in range(1, mats):
                @pl.when(now == m * per - 8)
                def _():
                    basis_copy(m).start()

                @pl.when(now == m * per)
                def _():
                    basis_copy(m).wait_recv()
                    turn(1, pair_b, m)

            def project(c):
                m, j = spot(c)
                raw_copy(c).wait_recv()
                mine = pl.ds(pl.multiple_of(j * chunk + y * half, half), half)
                theirs = pl.ds(pl.multiple_of(j * half, half), half)
                part[c % deep] = jnp.dot(
                    turned[0, m], gv[m, :, mine], preferred_element_type=f32
                ) + jnp.dot(turned[1, m], raw[m, :, theirs], preferred_element_type=f32)
                rs_sends(c, 0, start)

            stage(0, project)

            for t in range(1, hops):

                def middle(c, t=t):
                    rs_recv(c, t)
                    rs_sends(c, t, start)

                stage(t, middle)

            def complete(c):
                rs_recv(c, hops)
                keep = pl.ds(pl.multiple_of(z * band + y * height, height), height)
                dst = pl.ds(pl.multiple_of(y * half, half), half)
                proj_copy(c).start()
                proj[c % few, :, dst] = part[c % deep, keep, :]

            stage(hops, complete)

            @pl.when(now == 0)
            def _():
                sq_copy(0, (core_peer, row), 0).wait()
                sq_out[1] = sq_out[0] + sq_in[0]
                sq_copy(1, (x_peer, row), 1).start()

            @pl.when(now == 1)
            def _():
                sq_copy(1, (x_peer, row), 1).wait()
                sq_out[2] = sq_out[1] + sq_in[1]
                sq_copy(2, (me, y_peer), 2).start()

            @pl.when(now == 2)
            def _():
                sq_copy(2, (me, y_peer), 2).wait()
                sq_out[3] = sq_out[2] + sq_in[2]
                for d in range(1, line):
                    sq_line(d).start()

            @pl.when(now == 3)
            def _():
                whole = sq_out[3]
                for d in range(1, line):
                    sq_line(d).wait()
                    whole = whole + sq_in[2 + d]
                total = jnp.sum(whole, axis=(0, 1), keepdims=True)
                scale = limit / jnp.maximum(jnp.sqrt(total), limit)
                scale_v[...] = jnp.broadcast_to(scale, scale_v.shape)

            def step(c):
                m, j = spot(c)
                proj_copy(c).wait_recv()
                at = cols_at(j)
                first, second, update = moment_step(
                    proj[c % few], m1[m, :, at], m2[m, :, at], scale_v[0:1, 0:1]
                )
                m1[m, :, at] = first
                m2[m, :, at] = second
                upd[c % deep, own_rows(), :] = update
                upd_copy(c).start()

            stage(line, step)

            def spread(c):
                upd_copy(c).wait_recv()
                ag_sends(c, 0, start)

            stage(line + 1, spread)

            for t in range(1, hops):

                def relay(c, t=t):
                    ag_recv(c, t - 1)
                    ag_sends(c, t, start)

                stage(line + 1 + t, relay)

            def back(c):
                m, j = spot(c)
                ag_recv(c, hops - 1)
                product = jnp.dot(own_b[m], upd[c % deep], preferred_element_type=f32)
                fresh = wv[m, :, cols_at(j)].astype(f32) - 0.5 * product
                fresh_v[c % deep] = fresh.astype(bf16)
                x_copy(c, me).start()
                core_copy(c, me).start()
                own_copy(c).start()

            stage(back_lag, back)

            def forward(c):
                x_copy(c, x_peer).wait_recv()
                fwd_copy(c, x_peer).start()
                core_copy(c, core_peer).wait_recv()

            stage(back_lag + 2, forward)

            def last(c):
                fwd_copy(c, (core_peer + 2) % dp).wait_recv()
                fwd_copy(c, x_peer).wait_send()
                x_copy(c, me).wait_send()
                core_copy(c, me).wait_send()
                own_copy(c).wait()

            stage(back_lag + 3, last)

            for t in range(hops):

                def freed(c, t=t):
                    rs_sends(c, t, sent)

                stage(t + 2, freed)

                def freed_update(c, t=t):
                    ag_sends(c, t, sent)

                stage(line + 3 + t, freed_update)

            def freed_pair(c):
                raw_copy(c).wait_send()
                proj_copy(c).wait_send()

            stage(hops + 2, freed_pair)

            def freed_own(c):
                upd_copy(c).wait_send()

            stage(line + 2, freed_own)
            return carry

        lax.fori_loop(0, ticks, tick, 0)
        for m in range(mats):
            basis_copy(m).wait_send()
        stores = [
            pltpu.make_async_copy(m1, new_first, store.at[0]),
            pltpu.make_async_copy(m2, new_second, store.at[1]),
        ]
        for copy in stores:
            copy.start()
        for copy in stores:
            copy.wait()

    dma = pltpu.SemaphoreType.DMA
    anywhere = pl.BlockSpec(memory_space=pl.ANY)
    return pl.pallas_call(
        kernel,
        out_shape=(
            jax.ShapeDtypeStruct((mats, rows, cols * dp), bf16),
            jax.ShapeDtypeStruct(moment1.shape, f32),
            jax.ShapeDtypeStruct(moment2.shape, f32),
        ),
        in_specs=[anywhere] * 5,
        out_specs=(anywhere,) * 3,
        scratch_shapes=[
            pltpu.VMEM((mats, rows, cols), bf16),
            pltpu.VMEM((mats, rows, cols // 2), bf16),
            pltpu.VMEM((mats, rows, rank), bf16),
            pltpu.VMEM((mats, rows, rank), bf16),
            pltpu.VMEM((2, mats, rank, rows), bf16),
            pltpu.VMEM(moment1.shape, f32),
            pltpu.VMEM(moment2.shape, f32),
            pltpu.VMEM((mats, rows, cols), bf16),
            pltpu.VMEM((deep, rank, half), f32),
            pltpu.VMEM((few, hops, band, half), f32),
            pltpu.VMEM((few, hops, band, half), f32),
            pltpu.VMEM((few, height, chunk), f32),
            pltpu.VMEM((deep, rank, chunk), bf16),
            pltpu.VMEM((4, 8, 128), f32),
            pltpu.VMEM((2 + line, 8, 128), f32),
            pltpu.VMEM((8, 128), f32),
            dma((count,)), dma((count,)), dma((mats,)), dma((mats,)), dma((4 + mats,)),
            dma((2, few, hops)), dma((2, few, hops)), dma((few,)), dma((few,)),
            dma((few,)), dma((few,)), dma((2, few, hops)), dma((2, few, hops)),
            dma((deep,)), dma((deep,)), dma((deep,)), dma((deep,)),
            dma((deep,)), dma((deep,)), dma((2 + line,)), dma((2 + line,)), dma((2,)),
            pltpu.VMEM((deep, rows, chunk), bf16), dma((deep,)),
        ],
        compiler_params=pltpu.CompilerParams(
            collective_id=0, has_side_effects=True, vmem_limit_bytes=VMEM_LIMIT
        ),
        cost_estimate=pl.CostEstimate(
            flops=6 * mats * rows * rank * cols,
            bytes_accessed=8 * mats * rows * cols,
            transcendentals=0,
        ),
        name="step",
    )(grads, basis, moment1, moment2, weights)


def solution(mesh):
    dp = mesh.shape["dp"]
    cores = 2 if dp % 2 == 0 else 1
    chips = dp // cores
    n = mesh.shape["rows"]
    ring = [2 * q if q < n // 2 else 2 * (n - 1 - q) + 1 for q in range(n)]

    def sum_all(x):
        if dp & (dp - 1) or n & (n - 1):
            return lax.psum(x, ("dp", "rows"))
        x = jnp.full((8, 128), x, jnp.float32)
        for axis, size in (("rows", n), ("dp", dp)):
            bit = 1
            while bit < size:
                x = x + lax.ppermute(x, axis, [(i, i ^ bit) for i in range(size)])
                bit *= 2
        return x[0, 0]

    def local(grads, basis, moment1, moment2, weights):
        mats, rows, cols = grads.shape
        width = cols // SPLITS
        limit = 1.0 * math.sqrt(mats * rows * mesh.shape["rows"] * cols * dp)
        if dp == 4 and n == LONGEST_RING and cols % CHUNK == 0:
            return fused_step(
                mesh.shape, CHUNK, grads, basis, moment1, moment2, weights, limit
            )

        chunks = [(m, s) for m in range(mats) for s in range(SPLITS)]

        def part(x, m, s):
            return x[m, :, s * width : (s + 1) * width]

        partials = [
            lax.dot_general(
                basis[m],
                part(grads, m, s),
                (((0,), (0,)), ((), ())),
                preferred_element_type=jnp.float32,
            )
            for m, s in chunks
        ]
        wide = grads.astype(jnp.float32)
        total = sum_all(jnp.sum(wide * wide))
        scale = limit / jnp.maximum(jnp.sqrt(total), limit)

        me = lax.axis_index("dp")
        chip, core = me // cores, me % cores
        order = [(k, c) for c in range(cores) for k in range(chips)]
        groups = jnp.stack(
            [((chip + chips - k) % chips) * cores + (core + c) % cores for k, c in order]
        ).astype(jnp.int32)

        def from_chip(x, k):
            pairs = [
                (a * cores + c, ((a + k) % chips) * cores + c)
                for a in range(chips)
                for c in range(cores)
            ]
            return lax.ppermute(x, "dp", pairs)

        def from_core(x):
            pairs = [
                (a * cores + c, a * cores + (c + 1) % cores)
                for a in range(chips)
                for c in range(cores)
            ]
            return lax.ppermute(x, "dp", pairs)

        tie = lax.optimization_barrier
        row = lax.axis_index("rows")
        pos = jnp.where(row % 2 == 0, row // 2, n - 1 - row // 2)
        height = moment1.shape[1]

        def start_of(q):
            q = (q + 2 * n) % n
            return jnp.where(q < n // 2, 2 * q, 2 * (n - 1 - q) + 1) * height

        def hop(x, way):
            return lax.ppermute(
                x, "rows", [(ring[q], ring[(q + way) % n]) for q in range(n)]
            )

        def block(partial, q):
            return lax.dynamic_slice_in_dim(partial, start_of(q), height, 0)

        def hops_of(i):
            near, far = (n - 1) // 2, n // 2
            return ((1, far), (-1, near)) if i % 2 == 0 else ((1, near), (-1, far))

        def reduce_pair(held):
            if n > LONGEST_RING:
                return [
                    lax.psum_scatter(p, "rows", scatter_dimension=0, tiled=True)
                    for p in held
                ]
            sums = [block(p, pos) for p in held]
            live = {}
            for i, p in enumerate(held):
                for way, far in hops_of(i):
                    if far:
                        live[i, way] = block(p, pos + way * far)
            for step in range(n // 2):
                for i, p in enumerate(held):
                    for way, far in hops_of(i):
                        if step >= far:
                            continue
                        got = hop(live[i, way], way)
                        if step == far - 1:
                            sums[i] = sums[i] + got
                        else:
                            live[i, way] = got + block(p, pos + way * (far - 1 - step))
            return sums

        def gather_pair(held):
            if n > LONGEST_RING:
                return [lax.all_gather(x, "rows", axis=0, tiled=True) for x in held]
            full = []
            for x in held:
                empty = jnp.zeros((height * n, x.shape[1]), x.dtype)
                full.append(lax.dynamic_update_slice_in_dim(empty, x, row * height, 0))
            live = {(i, way): x for i, x in enumerate(held) for way in (1, -1)}
            for step in range(n // 2):
                for i in range(len(held)):
                    for way, far in hops_of(i):
                        if step >= far:
                            continue
                        live[i, way] = hop(live[i, way], way)
                        full[i] = lax.dynamic_update_slice_in_dim(
                            full[i], live[i, way], start_of(pos - way * (step + 1)), 0
                        )
            return full

        firsts, seconds, exchanged = [], [], []

        def finish(number, pair, sums):
            updates = []
            for (m, s), projected in zip(pair, sums):
                first, second, update = moment_step(
                    projected, part(moment1, m, s), part(moment2, m, s), scale
                )
                firsts.append(first)
                seconds.append(second)
                updates.append(update)
            for (m, s), full in zip(pair, gather_pair(updates)):
                back = jnp.dot(basis[m], full, preferred_element_type=jnp.float32)
                fresh = part(weights, m, s).astype(jnp.float32) - 0.5 * back
                fresh = fresh.astype(jnp.bfloat16)
                exchanged.append([fresh] + [from_chip(fresh, k) for k in range(1, chips)])

        sums = None
        pairs = [chunks[i : i + 2] for i in range(0, len(chunks), 2)]
        for number, pair in enumerate(pairs):
            held = partials[2 * number : 2 * number + 2]
            if sums is not None:
                held, sums = tie((held, sums))
            sums_before, sums = sums, reduce_pair(held)
            if number >= 1:
                finish(number - 1, pairs[number - 1], sums_before)
                sums, exchanged[-2][0], exchanged[-1][0] = tie(
                    (sums, exchanged[-2][0], exchanged[-1][0])
                )
        finish(len(pairs) - 1, pairs[-1], sums)

        shape = (mats, rows, cols * dp)
        count = len(chunks)
        out = None
        for i, (m, s) in enumerate(chunks):
            pieces = list(exchanged[i])
            if i < count - 2:
                pieces[1:], exchanged[-1][0] = tie((pieces[1:], exchanged[-1][0]))
            if i >= 2:
                pieces[1:], out = tie((pieces[1:], out))
            if cores == 2:
                pieces = pieces + [from_core(x) for x in pieces]
            out = place(groups, pieces, out, shape, m, s)

        def whole(parts):
            return jnp.stack(
                [
                    jnp.concatenate(parts[m * SPLITS : (m + 1) * SPLITS], axis=1)
                    for m in range(mats)
                ]
            )

        return (out, whole(firsts), whole(seconds))

    return jax.shard_map(
        local,
        mesh=mesh,
        in_specs=(
            P(None, "rows", "dp"),
            P(None, "rows", None),
            P(None, "rows", "dp"),
            P(None, "rows", "dp"),
            P(None, "rows", "dp"),
        ),
        out_specs=(P(None, "rows", None), P(None, "rows", "dp"), P(None, "rows", "dp")),
        check_vma=False,
    )
```

```python
import math

import jax
import jax.numpy as jnp
from jax import lax
from jax.experimental import pallas as pl
from jax.experimental.pallas import tpu as pltpu
from jax.sharding import PartitionSpec as P

STEP = 10
SPLITS = 2
LONGEST_RING = 8
CHUNK = 256
VMEM_LIMIT = 34 * 1024 * 1024


def moment_step(projected, moment1, moment2, scale):
    scaled = scale * projected
    first = 0.9 * moment1 + 0.1 * scaled
    second = 0.999 * moment2 + 0.001 * scaled * scaled
    first_bias_correction = 1.0 - 0.9**STEP
    second_fix = 1.0 - 0.999**STEP
    low_rank_update = (
        first / first_bias_correction / (jnp.sqrt(second / second_fix) + 1e-08)
    ).astype(jnp.bfloat16)
    return (first, second, low_rank_update)


def tile_of(width):
    tile = 128
    for cand in range(128, 1025, 128):
        if width % cand == 0:
            tile = cand
    return tile


def place(groups, pieces, out, shape, mat, split):
    count = len(pieces)
    rows, width = pieces[0].shape
    tile = tile_of(width)
    tiles = width // tile

    def piece_spec(p):
        def index(i, j, groups_ref):
            return (0, jnp.where(i == p, j, jnp.where(i < p, 0, tiles - 1)))

        return pl.BlockSpec((rows, tile), index)

    def out_index(i, j, groups_ref):
        return (mat, 0, groups_ref[i] * (SPLITS * tiles) + split * tiles + j)

    def kernel(groups_ref, *refs):
        out_ref = refs[-1]
        for p in range(count):

            @pl.when(pl.program_id(0) == p)
            def _():
                out_ref[0] = refs[p][...]

    extra = [] if out is None else [out]
    return pl.pallas_call(
        kernel,
        grid_spec=pltpu.PrefetchScalarGridSpec(
            num_scalar_prefetch=1,
            grid=(count, tiles),
            in_specs=[piece_spec(p) for p in range(count)]
            + [pl.BlockSpec(memory_space=pl.ANY) for _ in extra],
            out_specs=pl.BlockSpec((1, rows, tile), out_index),
        ),
        out_shape=jax.ShapeDtypeStruct(shape, pieces[0].dtype),
        input_output_aliases={} if out is None else {1 + count: 0},
        cost_estimate=pl.CostEstimate(
            flops=0, bytes_accessed=4 * count * rows * width, transcendentals=0
        ),
        name="place",
    )(groups, *pieces, *extra)


def fused_step(mesh_shape, chunk, grads, basis, moment1, moment2, weights, limit):
    mats, rows, cols = grads.shape
    rank = basis.shape[2]
    height = moment1.shape[1]
    dp = mesh_shape["dp"]
    line = mesh_shape["rows"] // 2
    band = 2 * height
    half = chunk // 2
    per = cols // chunk
    count = mats * per
    hops = line - 1
    ahead = 3
    deep, few = 8, 4
    back_lag = 2 * line
    ticks = count + back_lag + 4
    f32, bf16 = jnp.float32, jnp.bfloat16

    def kernel(
        grads_ref, basis_ref, first_ref, second_ref, weights_ref,
        out, new_first, new_second,
        gv, raw, own_b, pair_b, turned, m1, m2, wv,
        part, rup, rdn, proj, upd, sq_out, sq_in, scale_v,
        raw_s, raw_r, bas_s, bas_r, share_s, share_r, load, rs_s, rs_r, proj_s, proj_r,
        upd_s, upd_r, ag_s, ag_r, x_s, x_r, core_s, core_r, fwd_s, fwd_r,
        sq_s, sq_r, store,
    ):
        me, row = lax.axis_index("dp"), lax.axis_index("rows")
        z, y, core = row // 2, row % 2, me % 2
        flip = line - 1 - z
        core_peer = me + 1 - 2 * (me % 2)
        x_peer = (me + 2) % dp
        y_peer = row + 1 - 2 * y
        above = jnp.minimum(z + 1, line - 1) * 2 + y
        below = jnp.maximum(z - 1, 0) * 2 + y

        def remote(src, dst, s, r, device):
            return pltpu.make_async_remote_copy(
                src_ref=src, dst_ref=dst, send_sem=s, recv_sem=r,
                device_id=device, device_id_type=pl.DeviceIdType.MESH,
            )

        def rows_at(b):
            return pl.ds(pl.multiple_of(b * band, band), band)

        def spot(c):
            return c // per, c % per

        def cols_at(j):
            return pl.ds(pl.multiple_of(j * chunk, chunk), chunk)

        def out_at(owner, j):
            return pl.ds(pl.multiple_of(owner * cols + j * chunk, 128), chunk)

        def raw_copy(c):
            m, j = spot(c)
            src = pl.ds(pl.multiple_of(j * chunk + (1 - y) * half, half), half)
            dst = pl.ds(pl.multiple_of(j * half, half), half)
            return remote(
                grads_ref.at[m, :, src], raw.at[m, :, dst],
                raw_s.at[c], raw_r.at[c], (me, y_peer),
            )

        def basis_half(k):
            return pl.ds(pl.multiple_of(k * (rows // 2), rows // 2), rows // 2)

        def basis_copy(m):
            at = basis_half(core)
            return remote(
                basis_ref.at[m, at, :], pair_b.at[m, at, :],
                bas_s.at[m], bas_r.at[m], (me, y_peer),
            )

        def basis_share(m, k):
            ref = pair_b.at[m, basis_half(k), :]
            return remote(ref, ref, share_s.at[m], share_r.at[m], (core_peer, row))

        def up_block(t):
            return line - 1 - t + z

        def down_block(t):
            return t - line + 1 + z

        def rs_copy(c, t, way, b):
            slot = c % few
            buf, dev = (rup, above) if way == 0 else (rdn, below)
            return remote(
                part.at[c % deep, rows_at(b), :], buf.at[slot, t],
                rs_s.at[way, slot, t], rs_r.at[way, slot, t], (me, dev),
            )

        def rs_sends(c, t, act):
            @pl.when((z <= line - 2) & (z <= t))
            def _():
                act(rs_copy(c, t, 0, up_block(t)))

            @pl.when((z >= 1) & (flip <= t))
            def _():
                act(rs_copy(c, t, 1, down_block(t)))

        def rs_recv(c, t):
            slot = c % few

            @pl.when((z >= 1) & (z <= t))
            def _():
                rs_copy(c, t - 1, 0, z).wait_recv()
                b = rows_at(up_block(t))
                part[c % deep, b, :] = part[c % deep, b, :] + rup[slot, t - 1]

            @pl.when((flip >= 1) & (flip <= t))
            def _():
                rs_copy(c, t - 1, 1, z).wait_recv()
                b = rows_at(down_block(t))
                part[c % deep, b, :] = part[c % deep, b, :] + rdn[slot, t - 1]

        def proj_copy(c):
            src = pl.ds(pl.multiple_of(z * band + (1 - y) * height, height), height)
            dst = pl.ds(pl.multiple_of(y * half, half), half)
            return remote(
                part.at[c % deep, src, :], proj.at[c % few, :, dst],
                proj_s.at[c % few], proj_r.at[c % few], (me, y_peer),
            )

        def own_rows():
            return pl.ds(pl.multiple_of(row * height, height), height)

        def upd_copy(c):
            ref = upd.at[c % deep, own_rows(), :]
            return remote(ref, ref, upd_s.at[c % few], upd_r.at[c % few], (me, y_peer))

        def ag_copy(c, t, way, b):
            ref = upd.at[c % deep, rows_at(b), :]
            dev = above if way == 0 else below
            return remote(
                ref, ref, ag_s.at[way, c % few, t], ag_r.at[way, c % few, t], (me, dev)
            )

        def ag_sends(c, t, act):
            @pl.when((z <= line - 2) & (z >= t))
            def _():
                act(ag_copy(c, t, 0, z - t))

            @pl.when((z >= 1) & (z + t <= line - 1))
            def _():
                act(ag_copy(c, t, 1, z + t))

        def ag_recv(c, t):
            @pl.when(z >= t + 1)
            def _():
                ag_copy(c, t, 0, z - 1 - t).wait_recv()

            @pl.when(z + 1 + t <= line - 1)
            def _():
                ag_copy(c, t, 1, z + 1 + t).wait_recv()

        def x_copy(c, owner):
            m, j = spot(c)
            ref = out.at[m, :, out_at(owner, j)]
            return remote(ref, ref, x_s.at[c % deep], x_r.at[c % deep], (x_peer, row))

        def core_copy(c, owner):
            m, j = spot(c)
            ref = out.at[m, :, out_at(owner, j)]
            return remote(
                ref, ref, core_s.at[c % deep], core_r.at[c % deep], (core_peer, row)
            )

        def fwd_copy(c, owner):
            m, j = spot(c)
            ref = out.at[m, :, out_at(owner, j)]
            return remote(
                ref, ref, fwd_s.at[c % deep], fwd_r.at[c % deep], (core_peer, row)
            )

        def start(copy):
            copy.start()

        def sent(copy):
            copy.wait_send()

        loads = [
            pltpu.make_async_copy(basis_ref, own_b, load.at[0]),
            pltpu.make_async_copy(first_ref, m1, load.at[1]),
            pltpu.make_async_copy(second_ref, m2, load.at[2]),
            pltpu.make_async_copy(weights_ref, wv, load.at[3]),
        ]
        grad_loads = [
            pltpu.make_async_copy(grads_ref.at[m], gv.at[m], load.at[4 + m])
            for m in range(mats)
        ]
        loads[0].start()
        for copy in grad_loads:
            copy.start()
        for copy in loads[1:]:
            copy.start()

        barrier = pltpu.get_barrier_semaphore()
        peers = [(core_peer, row), (x_peer, row), (me, y_peer)] + [
            (me, ((z + d) % line) * 2 + y) for d in range(1, line)
        ]
        for device in peers:
            pl.semaphore_signal(
                barrier, inc=1, device_id=device, device_id_type=pl.DeviceIdType.MESH
            )
        pl.semaphore_wait(barrier, len(peers))

        basis_copy(0).start()
        for c in range(ahead):
            raw_copy(c).start()

        def turn(which, ref, m):
            for i in range(0, rows, 128):
                turned[which, m, :, i : i + 128] = ref[m, i : i + 128, :].T

        loads[0].wait()
        for m in range(mats):
            turn(0, own_b, m)

        squares = jnp.zeros((16, 128), f32)
        for m in range(mats):
            grad_loads[m].wait()

            def square(i, acc, m=m):
                wide = gv[m, pl.ds(pl.multiple_of(i * 16, 16), 16), :].astype(f32)
                wide = wide * wide
                for k in range(0, cols, 128):
                    acc = acc + wide[:, k : k + 128]
                return acc

            squares = lax.fori_loop(0, rows // 16, square, squares)
        sq_out[0] = squares[:8] + squares[8:]

        def sq_copy(k, device, slot):
            return remote(sq_out.at[k], sq_in.at[slot], sq_s.at[slot], sq_r.at[slot], device)

        def sq_line(d):
            return sq_copy(3, (me, ((z + d) % line) * 2 + y), 2 + d)

        basis_copy(0).wait_recv()
        basis_share(0, core).start()
        sq_copy(0, (core_peer, row), 0).start()
        for copy in loads[1:]:
            copy.wait()
        basis_share(0, 1 - core).wait_recv()
        turn(1, pair_b, 0)

        def tick(now, carry):
            def stage(lag, body):
                c = now - lag

                @pl.when((c >= 0) & (c < count))
                def _():
                    body(c)

            @pl.when(now + ahead < count)
            def _():
                raw_copy(now + ahead).start()

            for m in range(1, mats):

                @pl.when(now == max(m * per - 8, 0))
                def _():
                    basis_copy(m).start()

                @pl.when(now == max(m * per - 4, 1))
                def _():
                    basis_copy(m).wait_recv()
                    basis_share(m, core).start()

                @pl.when(now == m * per)
                def _():
                    basis_share(m, 1 - core).wait_recv()
                    turn(1, pair_b, m)

            def last(c):
                fwd_copy(c, (core_peer + 2) % dp).wait_recv()
                fwd_copy(c, x_peer).wait_send()
                x_copy(c, me).wait_send()
                core_copy(c, me).wait_send()

            stage(back_lag + 3, last)

            def forward(c):
                x_copy(c, x_peer).wait_recv()
                fwd_copy(c, x_peer).start()
                core_copy(c, core_peer).wait_recv()

            stage(back_lag + 2, forward)

            def back(c):
                m, j = spot(c)
                ag_recv(c, hops - 1)
                product = jnp.dot(own_b[m], upd[c % deep], preferred_element_type=f32)
                fresh = wv[m, :, cols_at(j)].astype(f32) - 0.5 * product
                out[m, :, out_at(me, j)] = fresh.astype(bf16)
                x_copy(c, me).start()
                core_copy(c, me).start()

            stage(back_lag, back)

            for t in range(hops - 1, 0, -1):

                def relay(c, t=t):
                    ag_recv(c, t - 1)
                    ag_sends(c, t, start)

                stage(line + 1 + t, relay)

            def spread(c):
                upd_copy(c).wait_recv()
                ag_sends(c, 0, start)

            stage(line + 1, spread)

            def step(c):
                m, j = spot(c)
                proj_copy(c).wait_recv()
                at = cols_at(j)
                first, second, update = moment_step(
                    proj[c % few], m1[m, :, at], m2[m, :, at], scale_v[0:1, 0:1]
                )
                upd[c % deep, own_rows(), :] = update
                upd_copy(c).start()
                m1[m, :, at] = first
                m2[m, :, at] = second

            stage(line, step)

            def complete(c):
                rs_recv(c, hops)
                keep = pl.ds(pl.multiple_of(z * band + y * height, height), height)
                dst = pl.ds(pl.multiple_of(y * half, half), half)
                proj_copy(c).start()
                proj[c % few, :, dst] = part[c % deep, keep, :]

            stage(hops, complete)

            for t in range(hops - 1, 0, -1):

                def middle(c, t=t):
                    rs_recv(c, t)
                    rs_sends(c, t, start)

                stage(t, middle)

            def project(c):
                m, j = spot(c)
                raw_copy(c).wait_recv()
                mine = pl.ds(pl.multiple_of(j * chunk + y * half, half), half)
                theirs = pl.ds(pl.multiple_of(j * half, half), half)
                part[c % deep] = jnp.dot(
                    turned[0, m], gv[m, :, mine], preferred_element_type=f32
                ) + jnp.dot(turned[1, m], raw[m, :, theirs], preferred_element_type=f32)
                rs_sends(c, 0, start)

            stage(0, project)

            @pl.when(now == 0)
            def _():
                sq_copy(0, (core_peer, row), 0).wait()
                sq_out[1] = sq_out[0] + sq_in[0]
                sq_copy(1, (x_peer, row), 1).start()

            @pl.when(now == 1)
            def _():
                sq_copy(1, (x_peer, row), 1).wait()
                sq_out[2] = sq_out[1] + sq_in[1]
                sq_copy(2, (me, y_peer), 2).start()

            @pl.when(now == 2)
            def _():
                sq_copy(2, (me, y_peer), 2).wait()
                sq_out[3] = sq_out[2] + sq_in[2]
                for d in range(1, line):
                    sq_line(d).start()

            @pl.when(now == 3)
            def _():
                whole = sq_out[3]
                for d in range(1, line):
                    sq_line(d).wait()
                    whole = whole + sq_in[2 + d]
                total = jnp.sum(whole, axis=(0, 1), keepdims=True)
                scale = limit / jnp.maximum(jnp.sqrt(total), limit)
                scale_v[...] = jnp.broadcast_to(scale, scale_v.shape)

            for t in range(hops):

                def freed(c, t=t):
                    rs_sends(c, t, sent)

                stage(t + 2, freed)

                def freed_update(c, t=t):
                    ag_sends(c, t, sent)

                stage(line + 3 + t, freed_update)

            def freed_pair(c):
                raw_copy(c).wait_send()
                proj_copy(c).wait_send()

            stage(hops + 2, freed_pair)

            def freed_own(c):
                upd_copy(c).wait_send()

            stage(line + 2, freed_own)
            return carry

        lax.fori_loop(0, ticks, tick, 0)
        for m in range(mats):
            basis_copy(m).wait_send()
            basis_share(m, core).wait_send()
        stores = [
            pltpu.make_async_copy(m1, new_first, store.at[0]),
            pltpu.make_async_copy(m2, new_second, store.at[1]),
        ]
        for copy in stores:
            copy.start()
        for copy in stores:
            copy.wait()

    dma = pltpu.SemaphoreType.DMA
    anywhere = pl.BlockSpec(memory_space=pl.ANY)
    fresh, first, second = pl.pallas_call(
        kernel,
        out_shape=(
            pltpu.VMEM((mats, rows, cols * dp), bf16),
            jax.ShapeDtypeStruct(moment1.shape, f32),
            jax.ShapeDtypeStruct(moment2.shape, f32),
        ),
        in_specs=[anywhere] * 5,
        out_specs=(pl.BlockSpec(memory_space=pltpu.VMEM), anywhere, anywhere),
        scratch_shapes=[
            pltpu.VMEM((mats, rows, cols), bf16),
            pltpu.VMEM((mats, rows, cols // 2), bf16),
            pltpu.VMEM((mats, rows, rank), bf16),
            pltpu.VMEM((mats, rows, rank), bf16),
            pltpu.VMEM((2, mats, rank, rows), bf16),
            pltpu.VMEM(moment1.shape, f32),
            pltpu.VMEM(moment2.shape, f32),
            pltpu.VMEM((mats, rows, cols), bf16),
            pltpu.VMEM((deep, rank, half), f32),
            pltpu.VMEM((few, hops, band, half), f32),
            pltpu.VMEM((few, hops, band, half), f32),
            pltpu.VMEM((few, height, chunk), f32),
            pltpu.VMEM((deep, rank, chunk), bf16),
            pltpu.VMEM((4, 8, 128), f32),
            pltpu.VMEM((2 + line, 8, 128), f32),
            pltpu.VMEM((8, 128), f32),
            dma((count,)), dma((count,)), dma((mats,)), dma((mats,)),
            dma((mats,)), dma((mats,)), dma((4 + mats,)),
            dma((2, few, hops)), dma((2, few, hops)), dma((few,)), dma((few,)),
            dma((few,)), dma((few,)), dma((2, few, hops)), dma((2, few, hops)),
            dma((deep,)), dma((deep,)), dma((deep,)), dma((deep,)),
            dma((deep,)), dma((deep,)), dma((2 + line,)), dma((2 + line,)), dma((2,)),
        ],
        compiler_params=pltpu.CompilerParams(
            collective_id=0, has_side_effects=True, vmem_limit_bytes=VMEM_LIMIT
        ),
        cost_estimate=pl.CostEstimate(
            flops=6 * mats * rows * rank * cols,
            bytes_accessed=8 * mats * rows * cols,
            transcendentals=0,
        ),
        name="step",
    )(grads, basis, moment1, moment2, weights)
    return settle(fresh), first, second


def settle(array):
    def kernel(source, target, done):
        copy = pltpu.make_async_copy(source, target, done)
        copy.start()
        copy.wait()

    return pl.pallas_call(
        kernel,
        out_shape=jax.ShapeDtypeStruct(array.shape, array.dtype),
        in_specs=[pl.BlockSpec(memory_space=pltpu.VMEM)],
        out_specs=pl.BlockSpec(memory_space=pl.ANY),
        scratch_shapes=[pltpu.SemaphoreType.DMA],
        compiler_params=pltpu.CompilerParams(vmem_limit_bytes=1024 * 1024),
        name="settle",
    )(array)


def solution(mesh):
    dp = mesh.shape["dp"]
    cores = 2 if dp % 2 == 0 else 1
    chips = dp // cores
    n = mesh.shape["rows"]
    ring = [2 * q if q < n // 2 else 2 * (n - 1 - q) + 1 for q in range(n)]

    def sum_all(x):
        if dp & (dp - 1) or n & (n - 1):
            return lax.psum(x, ("dp", "rows"))
        x = jnp.full((8, 128), x, jnp.float32)
        for axis, size in (("rows", n), ("dp", dp)):
            bit = 1
            while bit < size:
                x = x + lax.ppermute(x, axis, [(i, i ^ bit) for i in range(size)])
                bit *= 2
        return x[0, 0]

    def local(grads, basis, moment1, moment2, weights):
        mats, rows, cols = grads.shape
        width = cols // SPLITS
        limit = 1.0 * math.sqrt(mats * rows * mesh.shape["rows"] * cols * dp)
        if dp == 4 and n == LONGEST_RING and cols % CHUNK == 0:
            return fused_step(
                mesh.shape, CHUNK, grads, basis, moment1, moment2, weights, limit
            )

        chunks = [(m, s) for m in range(mats) for s in range(SPLITS)]

        def part(x, m, s):
            return x[m, :, s * width : (s + 1) * width]

        partials = [
            lax.dot_general(
                basis[m],
                part(grads, m, s),
                (((0,), (0,)), ((), ())),
                preferred_element_type=jnp.float32,
            )
            for m, s in chunks
        ]
        wide = grads.astype(jnp.float32)
        total = sum_all(jnp.sum(wide * wide))
        scale = limit / jnp.maximum(jnp.sqrt(total), limit)

        me = lax.axis_index("dp")
        chip, core = me // cores, me % cores
        order = [(k, c) for c in range(cores) for k in range(chips)]
        groups = jnp.stack(
            [((chip + chips - k) % chips) * cores + (core + c) % cores for k, c in order]
        ).astype(jnp.int32)

        def from_chip(x, k):
            pairs = [
                (a * cores + c, ((a + k) % chips) * cores + c)
                for a in range(chips)
                for c in range(cores)
            ]
            return lax.ppermute(x, "dp", pairs)

        def from_core(x):
            pairs = [
                (a * cores + c, a * cores + (c + 1) % cores)
                for a in range(chips)
                for c in range(cores)
            ]
            return lax.ppermute(x, "dp", pairs)

        tie = lax.optimization_barrier
        row = lax.axis_index("rows")
        pos = jnp.where(row % 2 == 0, row // 2, n - 1 - row // 2)
        height = moment1.shape[1]

        def start_of(q):
            q = (q + 2 * n) % n
            return jnp.where(q < n // 2, 2 * q, 2 * (n - 1 - q) + 1) * height

        def hop(x, way):
            return lax.ppermute(
                x, "rows", [(ring[q], ring[(q + way) % n]) for q in range(n)]
            )

        def block(partial, q):
            return lax.dynamic_slice_in_dim(partial, start_of(q), height, 0)

        def hops_of(i):
            near, far = (n - 1) // 2, n // 2
            return ((1, far), (-1, near)) if i % 2 == 0 else ((1, near), (-1, far))

        def reduce_pair(held):
            if n > LONGEST_RING:
                return [
                    lax.psum_scatter(p, "rows", scatter_dimension=0, tiled=True)
                    for p in held
                ]
            sums = [block(p, pos) for p in held]
            live = {}
            for i, p in enumerate(held):
                for way, far in hops_of(i):
                    if far:
                        live[i, way] = block(p, pos + way * far)
            for step in range(n // 2):
                for i, p in enumerate(held):
                    for way, far in hops_of(i):
                        if step >= far:
                            continue
                        got = hop(live[i, way], way)
                        if step == far - 1:
                            sums[i] = sums[i] + got
                        else:
                            live[i, way] = got + block(p, pos + way * (far - 1 - step))
            return sums

        def gather_pair(held):
            if n > LONGEST_RING:
                return [lax.all_gather(x, "rows", axis=0, tiled=True) for x in held]
            full = []
            for x in held:
                empty = jnp.zeros((height * n, x.shape[1]), x.dtype)
                full.append(lax.dynamic_update_slice_in_dim(empty, x, row * height, 0))
            live = {(i, way): x for i, x in enumerate(held) for way in (1, -1)}
            for step in range(n // 2):
                for i in range(len(held)):
                    for way, far in hops_of(i):
                        if step >= far:
                            continue
                        live[i, way] = hop(live[i, way], way)
                        full[i] = lax.dynamic_update_slice_in_dim(
                            full[i], live[i, way], start_of(pos - way * (step + 1)), 0
                        )
            return full

        firsts, seconds, exchanged = [], [], []

        def finish(number, pair, sums):
            updates = []
            for (m, s), projected in zip(pair, sums):
                first, second, update = moment_step(
                    projected, part(moment1, m, s), part(moment2, m, s), scale
                )
                firsts.append(first)
                seconds.append(second)
                updates.append(update)
            for (m, s), full in zip(pair, gather_pair(updates)):
                back = jnp.dot(basis[m], full, preferred_element_type=jnp.float32)
                fresh = part(weights, m, s).astype(jnp.float32) - 0.5 * back
                fresh = fresh.astype(jnp.bfloat16)
                exchanged.append([fresh] + [from_chip(fresh, k) for k in range(1, chips)])

        sums = None
        pairs = [chunks[i : i + 2] for i in range(0, len(chunks), 2)]
        for number, pair in enumerate(pairs):
            held = partials[2 * number : 2 * number + 2]
            if sums is not None:
                held, sums = tie((held, sums))
            sums_before, sums = sums, reduce_pair(held)
            if number >= 1:
                finish(number - 1, pairs[number - 1], sums_before)
                sums, exchanged[-2][0], exchanged[-1][0] = tie(
                    (sums, exchanged[-2][0], exchanged[-1][0])
                )
        finish(len(pairs) - 1, pairs[-1], sums)

        shape = (mats, rows, cols * dp)
        count = len(chunks)
        out = None
        for i, (m, s) in enumerate(chunks):
            pieces = list(exchanged[i])
            if i < count - 2:
                pieces[1:], exchanged[-1][0] = tie((pieces[1:], exchanged[-1][0]))
            if i >= 2:
                pieces[1:], out = tie((pieces[1:], out))
            if cores == 2:
                pieces = pieces + [from_core(x) for x in pieces]
            out = place(groups, pieces, out, shape, m, s)

        def whole(parts):
            return jnp.stack(
                [
                    jnp.concatenate(parts[m * SPLITS : (m + 1) * SPLITS], axis=1)
                    for m in range(mats)
                ]
            )

        return (out, whole(firsts), whole(seconds))

    return jax.shard_map(
        local,
        mesh=mesh,
        in_specs=(
            P(None, "rows", "dp"),
            P(None, "rows", None),
            P(None, "rows", "dp"),
            P(None, "rows", "dp"),
            P(None, "rows", "dp"),
        ),
        out_specs=(P(None, "rows", None), P(None, "rows", "dp"), P(None, "rows", "dp")),
        check_vma=False,
    )
```

```python
import math

import jax
import jax.numpy as jnp
from jax import lax
from jax.experimental import pallas as pl
from jax.experimental.pallas import tpu as pltpu
from jax.sharding import PartitionSpec as P

STEP = 10
SPLITS = 2
LONGEST_RING = 8
CHUNK = 256
VMEM_LIMIT = 31 * 1024 * 1024


def moment_step(projected, moment1, moment2, scale):
    scaled = scale * projected
    first = 0.9 * moment1 + 0.1 * scaled
    second = 0.999 * moment2 + 0.001 * scaled * scaled
    first_bias_correction = 1.0 - 0.9**STEP
    second_fix = 1.0 - 0.999**STEP
    low_rank_update = (
        first / first_bias_correction / (jnp.sqrt(second / second_fix) + 1e-08)
    ).astype(jnp.bfloat16)
    return (first, second, low_rank_update)


def tile_of(width):
    tile = 128
    for cand in range(128, 1025, 128):
        if width % cand == 0:
            tile = cand
    return tile


def place(groups, pieces, out, shape, mat, split):
    count = len(pieces)
    rows, width = pieces[0].shape
    tile = tile_of(width)
    tiles = width // tile

    def piece_spec(p):
        def index(i, j, groups_ref):
            return (0, jnp.where(i == p, j, jnp.where(i < p, 0, tiles - 1)))

        return pl.BlockSpec((rows, tile), index)

    def out_index(i, j, groups_ref):
        return (mat, 0, groups_ref[i] * (SPLITS * tiles) + split * tiles + j)

    def kernel(groups_ref, *refs):
        out_ref = refs[-1]
        for p in range(count):

            @pl.when(pl.program_id(0) == p)
            def _():
                out_ref[0] = refs[p][...]

    extra = [] if out is None else [out]
    return pl.pallas_call(
        kernel,
        grid_spec=pltpu.PrefetchScalarGridSpec(
            num_scalar_prefetch=1,
            grid=(count, tiles),
            in_specs=[piece_spec(p) for p in range(count)]
            + [pl.BlockSpec(memory_space=pl.ANY) for _ in extra],
            out_specs=pl.BlockSpec((1, rows, tile), out_index),
        ),
        out_shape=jax.ShapeDtypeStruct(shape, pieces[0].dtype),
        input_output_aliases={} if out is None else {1 + count: 0},
        cost_estimate=pl.CostEstimate(
            flops=0, bytes_accessed=4 * count * rows * width, transcendentals=0
        ),
        name="place",
    )(groups, *pieces, *extra)


def fused_step(mesh_shape, chunk, grads, basis, moment1, moment2, weights, limit):
    mats, rows, cols = grads.shape
    rank = basis.shape[2]
    height = moment1.shape[1]
    dp = mesh_shape["dp"]
    line = mesh_shape["rows"] // 2
    band = 2 * height
    half = chunk // 2
    per = cols // chunk
    count = mats * per
    hops = line - 1
    ahead = 2
    deep, few, cuts = 8, 4, 4
    back_lag = 2 * line
    ticks = count + back_lag + 4
    f32, bf16 = jnp.float32, jnp.bfloat16

    def kernel(
        grads_ref, basis_ref, first_ref, second_ref, weights_ref,
        out, m1, m2,
        gv, raw, own_b, pair_b, turned, wv,
        part, rup, rdn, proj, upd, sq_out, sq_in, scale_v,
        raw_s, raw_r, bas_s, bas_r, share_s, share_r, load, rs_s, rs_r, proj_s, proj_r,
        upd_s, upd_r, ag_s, ag_r, x_s, x_r, core_s, core_r, fwd_s, fwd_r,
        sq_s, sq_r,
    ):
        me, row = lax.axis_index("dp"), lax.axis_index("rows")
        z, y, core = row // 2, row % 2, me % 2
        flip = line - 1 - z
        core_peer = me + 1 - 2 * (me % 2)
        x_peer = (me + 2) % dp
        y_peer = row + 1 - 2 * y
        above = jnp.minimum(z + 1, line - 1) * 2 + y
        below = jnp.maximum(z - 1, 0) * 2 + y

        def remote(src, dst, s, r, device):
            return pltpu.make_async_remote_copy(
                src_ref=src, dst_ref=dst, send_sem=s, recv_sem=r,
                device_id=device, device_id_type=pl.DeviceIdType.MESH,
            )

        def rows_at(b):
            return pl.ds(pl.multiple_of(b * band, band), band)

        def spot(c):
            return c // per, c % per

        def cols_at(j):
            return pl.ds(pl.multiple_of(j * chunk, chunk), chunk)

        def out_at(owner, j):
            return pl.ds(pl.multiple_of(owner * cols + j * chunk, 128), chunk)

        def raw_copy(c):
            m, j = spot(c)
            src = pl.ds(pl.multiple_of(j * chunk + (1 - y) * half, half), half)
            dst = pl.ds(pl.multiple_of(j * half, half), half)
            return remote(
                grads_ref.at[m, :, src], raw.at[m, :, dst],
                raw_s.at[c], raw_r.at[c], (me, y_peer),
            )

        def basis_half(k):
            return pl.ds(pl.multiple_of(k * (rows // 2), rows // 2), rows // 2)

        def basis_copy(m, q):
            size = rows // 2 // cuts
            at = pl.ds(pl.multiple_of(core * (rows // 2) + q * size, size), size)
            return remote(
                basis_ref.at[m, at, :], pair_b.at[m, at, :],
                bas_s.at[m, q], bas_r.at[m, q], (me, y_peer),
            )

        def basis_share(m, k):
            ref = pair_b.at[m, basis_half(k), :]
            return remote(ref, ref, share_s.at[m], share_r.at[m], (core_peer, row))

        def up_block(t):
            return line - 1 - t + z

        def down_block(t):
            return t - line + 1 + z

        def rs_copy(c, t, way, b):
            slot = c % few
            buf, dev = (rup, above) if way == 0 else (rdn, below)
            return remote(
                part.at[c % deep, rows_at(b), :], buf.at[slot, t],
                rs_s.at[way, slot, t], rs_r.at[way, slot, t], (me, dev),
            )

        def rs_sends(c, t, act):
            @pl.when((z <= line - 2) & (z <= t))
            def _():
                act(rs_copy(c, t, 0, up_block(t)))

            @pl.when((z >= 1) & (flip <= t))
            def _():
                act(rs_copy(c, t, 1, down_block(t)))

        def rs_recv(c, t):
            slot = c % few

            @pl.when((z >= 1) & (z <= t))
            def _():
                rs_copy(c, t - 1, 0, z).wait_recv()
                b = rows_at(up_block(t))
                part[c % deep, b, :] = part[c % deep, b, :] + rup[slot, t - 1]

            @pl.when((flip >= 1) & (flip <= t))
            def _():
                rs_copy(c, t - 1, 1, z).wait_recv()
                b = rows_at(down_block(t))
                part[c % deep, b, :] = part[c % deep, b, :] + rdn[slot, t - 1]

        def proj_copy(c):
            src = pl.ds(pl.multiple_of(z * band + (1 - y) * height, height), height)
            dst = pl.ds(pl.multiple_of(y * half, half), half)
            return remote(
                part.at[c % deep, src, :], proj.at[c % few, :, dst],
                proj_s.at[c % few], proj_r.at[c % few], (me, y_peer),
            )

        def own_rows():
            return pl.ds(pl.multiple_of(row * height, height), height)

        def upd_copy(c):
            ref = upd.at[c % deep, own_rows(), :]
            return remote(ref, ref, upd_s.at[c % few], upd_r.at[c % few], (me, y_peer))

        def ag_copy(c, t, way, b):
            ref = upd.at[c % deep, rows_at(b), :]
            dev = above if way == 0 else below
            return remote(
                ref, ref, ag_s.at[way, c % few, t], ag_r.at[way, c % few, t], (me, dev)
            )

        def ag_sends(c, t, act):
            @pl.when((z <= line - 2) & (z >= t))
            def _():
                act(ag_copy(c, t, 0, z - t))

            @pl.when((z >= 1) & (z + t <= line - 1))
            def _():
                act(ag_copy(c, t, 1, z + t))

        def ag_recv(c, t):
            @pl.when(z >= t + 1)
            def _():
                ag_copy(c, t, 0, z - 1 - t).wait_recv()

            @pl.when(z + 1 + t <= line - 1)
            def _():
                ag_copy(c, t, 1, z + 1 + t).wait_recv()

        def x_copy(c, owner):
            m, j = spot(c)
            ref = out.at[m, :, out_at(owner, j)]
            return remote(ref, ref, x_s.at[c % deep], x_r.at[c % deep], (x_peer, row))

        def core_copy(c, owner):
            m, j = spot(c)
            ref = out.at[m, :, out_at(owner, j)]
            return remote(
                ref, ref, core_s.at[c % deep], core_r.at[c % deep], (core_peer, row)
            )

        def fwd_copy(c, owner):
            m, j = spot(c)
            ref = out.at[m, :, out_at(owner, j)]
            return remote(
                ref, ref, fwd_s.at[c % deep], fwd_r.at[c % deep], (core_peer, row)
            )

        def start(copy):
            copy.start()

        def sent(copy):
            copy.wait_send()

        loads = [
            pltpu.make_async_copy(basis_ref, own_b, load.at[0]),
            pltpu.make_async_copy(first_ref, m1, load.at[1]),
            pltpu.make_async_copy(second_ref, m2, load.at[2]),
            pltpu.make_async_copy(weights_ref, wv, load.at[3]),
        ]
        grad_loads = [
            pltpu.make_async_copy(grads_ref.at[m], gv.at[m], load.at[4 + m])
            for m in range(mats)
        ]
        loads[0].start()
        for copy in grad_loads:
            copy.start()
        for copy in loads[1:]:
            copy.start()

        barrier = pltpu.get_barrier_semaphore()
        peers = [(core_peer, row), (x_peer, row), (me, y_peer)] + [
            (me, ((z + d) % line) * 2 + y) for d in range(1, line)
        ]
        for device in peers:
            pl.semaphore_signal(
                barrier, inc=1, device_id=device, device_id_type=pl.DeviceIdType.MESH
            )
        pl.semaphore_wait(barrier, len(peers))

        for q in range(cuts):
            basis_copy(0, q).start()
        for c in range(ahead):
            raw_copy(c).start()

        def turn(which, ref, m):
            for i in range(0, rows, 128):
                turned[which, m, :, i : i + 128] = ref[m, i : i + 128, :].T

        loads[0].wait()
        for m in range(mats):
            turn(0, own_b, m)

        squares = jnp.zeros((16, 128), f32)
        for m in range(mats):
            grad_loads[m].wait()

            def square(i, acc, m=m):
                wide = gv[m, pl.ds(pl.multiple_of(i * 16, 16), 16), :].astype(f32)
                wide = wide * wide
                for k in range(0, cols, 128):
                    acc = acc + wide[:, k : k + 128]
                return acc

            squares = lax.fori_loop(0, rows // 16, square, squares)
        sq_out[0] = squares[:8] + squares[8:]

        def sq_copy(k, device, slot):
            return remote(sq_out.at[k], sq_in.at[slot], sq_s.at[slot], sq_r.at[slot], device)

        def sq_line(d):
            return sq_copy(3, (me, ((z + d) % line) * 2 + y), 2 + d)

        for q in range(cuts):
            basis_copy(0, q).wait_recv()
        basis_share(0, core).start()
        sq_copy(0, (core_peer, row), 0).start()
        for copy in loads[1:]:
            copy.wait()
        basis_share(0, 1 - core).wait_recv()
        turn(1, pair_b, 0)

        def tick(now, carry):
            def stage(lag, body):
                c = now - lag

                @pl.when((c >= 0) & (c < count))
                def _():
                    body(c)

            for m in range(1, mats):

                for q in range(cuts):

                    @pl.when(now == max(m * per - 2 * cuts - 3 + 2 * q, 0))
                    def _():
                        basis_copy(m, q).start()

                @pl.when(now == max(m * per - 3, 1))
                def _():
                    for q in range(cuts):
                        basis_copy(m, q).wait_recv()
                    basis_share(m, core).start()

                @pl.when(now == m * per)
                def _():
                    basis_share(m, 1 - core).wait_recv()
                    turn(1, pair_b, m)

            def last(c):
                fwd_copy(c, (core_peer + 2) % dp).wait_recv()
                fwd_copy(c, x_peer).wait_send()
                x_copy(c, me).wait_send()
                core_copy(c, me).wait_send()

            stage(back_lag + 3, last)

            def forward(c):
                x_copy(c, x_peer).wait_recv()
                fwd_copy(c, x_peer).start()
                core_copy(c, core_peer).wait_recv()

            stage(back_lag + 2, forward)

            def back(c):
                m, j = spot(c)
                ag_recv(c, hops - 1)
                product = jnp.dot(own_b[m], upd[c % deep], preferred_element_type=f32)
                fresh = wv[m, :, cols_at(j)].astype(f32) - 0.5 * product
                out[m, :, out_at(me, j)] = fresh.astype(bf16)
                x_copy(c, me).start()
                core_copy(c, me).start()

            stage(back_lag, back)

            for t in range(hops - 1, 0, -1):

                def relay(c, t=t):
                    ag_recv(c, t - 1)
                    ag_sends(c, t, start)

                stage(line + 1 + t, relay)

            def spread(c):
                upd_copy(c).wait_recv()
                ag_sends(c, 0, start)

            stage(line + 1, spread)

            def step(c):
                m, j = spot(c)
                proj_copy(c).wait_recv()
                at = cols_at(j)
                first, second, update = moment_step(
                    proj[c % few], m1[m, :, at], m2[m, :, at], scale_v[0:1, 0:1]
                )
                upd[c % deep, own_rows(), :] = update
                upd_copy(c).start()
                m1[m, :, at] = first
                m2[m, :, at] = second

            stage(line, step)

            def complete(c):
                rs_recv(c, hops)
                keep = pl.ds(pl.multiple_of(z * band + y * height, height), height)
                dst = pl.ds(pl.multiple_of(y * half, half), half)
                proj_copy(c).start()
                proj[c % few, :, dst] = part[c % deep, keep, :]

            stage(hops, complete)

            for t in range(hops - 1, 0, -1):

                def middle(c, t=t):
                    rs_recv(c, t)
                    rs_sends(c, t, start)

                stage(t, middle)

            def project(c):
                m, j = spot(c)
                raw_copy(c).wait_recv()
                mine = pl.ds(pl.multiple_of(j * chunk + y * half, half), half)
                theirs = pl.ds(pl.multiple_of(j * half, half), half)
                part[c % deep] = jnp.dot(
                    turned[0, m], gv[m, :, mine], preferred_element_type=f32
                ) + jnp.dot(turned[1, m], raw[m, :, theirs], preferred_element_type=f32)
                rs_sends(c, 0, start)

            stage(0, project)

            @pl.when(now + ahead < count)
            def _():
                raw_copy(now + ahead).start()

            @pl.when(now == 0)
            def _():
                sq_copy(0, (core_peer, row), 0).wait()
                sq_out[1] = sq_out[0] + sq_in[0]
                sq_copy(1, (x_peer, row), 1).start()

            @pl.when(now == 1)
            def _():
                sq_copy(1, (x_peer, row), 1).wait()
                sq_out[2] = sq_out[1] + sq_in[1]
                sq_copy(2, (me, y_peer), 2).start()

            @pl.when(now == 2)
            def _():
                sq_copy(2, (me, y_peer), 2).wait()
                sq_out[3] = sq_out[2] + sq_in[2]
                for d in range(1, line):
                    sq_line(d).start()

            @pl.when(now == 3)
            def _():
                whole = sq_out[3]
                for d in range(1, line):
                    sq_line(d).wait()
                    whole = whole + sq_in[2 + d]
                total = jnp.sum(whole, axis=(0, 1), keepdims=True)
                scale = limit / jnp.maximum(jnp.sqrt(total), limit)
                scale_v[...] = jnp.broadcast_to(scale, scale_v.shape)

            for t in range(hops):

                def freed(c, t=t):
                    rs_sends(c, t, sent)

                stage(t + 2, freed)

                def freed_update(c, t=t):
                    ag_sends(c, t, sent)

                stage(line + 3 + t, freed_update)

            def freed_pair(c):
                raw_copy(c).wait_send()
                proj_copy(c).wait_send()

            stage(hops + 2, freed_pair)

            def freed_own(c):
                upd_copy(c).wait_send()

            stage(line + 2, freed_own)
            return carry

        lax.fori_loop(0, ticks, tick, 0)
        for m in range(mats):
            for q in range(cuts):
                basis_copy(m, q).wait_send()
            basis_share(m, core).wait_send()

    dma = pltpu.SemaphoreType.DMA
    anywhere = pl.BlockSpec(memory_space=pl.ANY)
    fresh, first, second = pl.pallas_call(
        kernel,
        out_shape=(
            pltpu.VMEM((mats, rows, cols * dp), bf16),
            pltpu.VMEM(moment1.shape, f32),
            pltpu.VMEM(moment2.shape, f32),
        ),
        in_specs=[anywhere] * 5,
        out_specs=(pl.BlockSpec(memory_space=pltpu.VMEM),) * 3,
        scratch_shapes=[
            pltpu.VMEM((mats, rows, cols), bf16),
            pltpu.VMEM((mats, rows, cols // 2), bf16),
            pltpu.VMEM((mats, rows, rank), bf16),
            pltpu.VMEM((mats, rows, rank), bf16),
            pltpu.VMEM((2, mats, rank, rows), bf16),
            pltpu.VMEM((mats, rows, cols), bf16),
            pltpu.VMEM((deep, rank, half), f32),
            pltpu.VMEM((few, hops, band, half), f32),
            pltpu.VMEM((few, hops, band, half), f32),
            pltpu.VMEM((few, height, chunk), f32),
            pltpu.VMEM((deep, rank, chunk), bf16),
            pltpu.VMEM((4, 8, 128), f32),
            pltpu.VMEM((2 + line, 8, 128), f32),
            pltpu.VMEM((8, 128), f32),
            dma((count,)), dma((count,)), dma((mats, cuts)), dma((mats, cuts)),
            dma((mats,)), dma((mats,)), dma((4 + mats,)),
            dma((2, few, hops)), dma((2, few, hops)), dma((few,)), dma((few,)),
            dma((few,)), dma((few,)), dma((2, few, hops)), dma((2, few, hops)),
            dma((deep,)), dma((deep,)), dma((deep,)), dma((deep,)),
            dma((deep,)), dma((deep,)), dma((2 + line,)), dma((2 + line,)),
        ],
        compiler_params=pltpu.CompilerParams(
            collective_id=0, has_side_effects=True, vmem_limit_bytes=VMEM_LIMIT
        ),
        cost_estimate=pl.CostEstimate(
            flops=6 * mats * rows * rank * cols,
            bytes_accessed=8 * mats * rows * cols,
            transcendentals=0,
        ),
        name="step",
    )(grads, basis, moment1, moment2, weights)
    (fresh,) = settle((fresh,), 4)
    return (fresh, *settle((first, second), 1))


def settle(arrays, cuts):
    count = len(arrays)

    def kernel(*refs):
        done = refs[-1]
        copies = []
        for i in range(count):
            size = arrays[i].shape[1] // cuts
            for m in range(arrays[i].shape[0]):
                for k in range(cuts):
                    at = pl.ds(k * size, size)
                    copies.append(
                        pltpu.make_async_copy(
                            refs[i].at[m, at, :],
                            refs[count + i].at[m, at, :],
                            done.at[len(copies)],
                        )
                    )
        for copy in copies:
            copy.start()
        for copy in copies:
            copy.wait()

    return pl.pallas_call(
        kernel,
        out_shape=tuple(jax.ShapeDtypeStruct(x.shape, x.dtype) for x in arrays),
        in_specs=[pl.BlockSpec(memory_space=pltpu.VMEM)] * count,
        out_specs=(pl.BlockSpec(memory_space=pl.ANY),) * count,
        scratch_shapes=[
            pltpu.SemaphoreType.DMA((cuts * sum(x.shape[0] for x in arrays),))
        ],
        compiler_params=pltpu.CompilerParams(vmem_limit_bytes=1024 * 1024),
        name="settle",
    )(*arrays)


def solution(mesh):
    dp = mesh.shape["dp"]
    cores = 2 if dp % 2 == 0 else 1
    chips = dp // cores
    n = mesh.shape["rows"]
    ring = [2 * q if q < n // 2 else 2 * (n - 1 - q) + 1 for q in range(n)]

    def sum_all(x):
        if dp & (dp - 1) or n & (n - 1):
            return lax.psum(x, ("dp", "rows"))
        x = jnp.full((8, 128), x, jnp.float32)
        for axis, size in (("rows", n), ("dp", dp)):
            bit = 1
            while bit < size:
                x = x + lax.ppermute(x, axis, [(i, i ^ bit) for i in range(size)])
                bit *= 2
        return x[0, 0]

    def local(grads, basis, moment1, moment2, weights):
        mats, rows, cols = grads.shape
        width = cols // SPLITS
        limit = 1.0 * math.sqrt(mats * rows * mesh.shape["rows"] * cols * dp)
        if dp == 4 and n == LONGEST_RING and cols % CHUNK == 0:
            return fused_step(
                mesh.shape, CHUNK, grads, basis, moment1, moment2, weights, limit
            )

        chunks = [(m, s) for m in range(mats) for s in range(SPLITS)]

        def part(x, m, s):
            return x[m, :, s * width : (s + 1) * width]

        partials = [
            lax.dot_general(
                basis[m],
                part(grads, m, s),
                (((0,), (0,)), ((), ())),
                preferred_element_type=jnp.float32,
            )
            for m, s in chunks
        ]
        wide = grads.astype(jnp.float32)
        total = sum_all(jnp.sum(wide * wide))
        scale = limit / jnp.maximum(jnp.sqrt(total), limit)

        me = lax.axis_index("dp")
        chip, core = me // cores, me % cores
        order = [(k, c) for c in range(cores) for k in range(chips)]
        groups = jnp.stack(
            [((chip + chips - k) % chips) * cores + (core + c) % cores for k, c in order]
        ).astype(jnp.int32)

        def from_chip(x, k):
            pairs = [
                (a * cores + c, ((a + k) % chips) * cores + c)
                for a in range(chips)
                for c in range(cores)
            ]
            return lax.ppermute(x, "dp", pairs)

        def from_core(x):
            pairs = [
                (a * cores + c, a * cores + (c + 1) % cores)
                for a in range(chips)
                for c in range(cores)
            ]
            return lax.ppermute(x, "dp", pairs)

        tie = lax.optimization_barrier
        row = lax.axis_index("rows")
        pos = jnp.where(row % 2 == 0, row // 2, n - 1 - row // 2)
        height = moment1.shape[1]

        def start_of(q):
            q = (q + 2 * n) % n
            return jnp.where(q < n // 2, 2 * q, 2 * (n - 1 - q) + 1) * height

        def hop(x, way):
            return lax.ppermute(
                x, "rows", [(ring[q], ring[(q + way) % n]) for q in range(n)]
            )

        def block(partial, q):
            return lax.dynamic_slice_in_dim(partial, start_of(q), height, 0)

        def hops_of(i):
            near, far = (n - 1) // 2, n // 2
            return ((1, far), (-1, near)) if i % 2 == 0 else ((1, near), (-1, far))

        def reduce_pair(held):
            if n > LONGEST_RING:
                return [
                    lax.psum_scatter(p, "rows", scatter_dimension=0, tiled=True)
                    for p in held
                ]
            sums = [block(p, pos) for p in held]
            live = {}
            for i, p in enumerate(held):
                for way, far in hops_of(i):
                    if far:
                        live[i, way] = block(p, pos + way * far)
            for step in range(n // 2):
                for i, p in enumerate(held):
                    for way, far in hops_of(i):
                        if step >= far:
                            continue
                        got = hop(live[i, way], way)
                        if step == far - 1:
                            sums[i] = sums[i] + got
                        else:
                            live[i, way] = got + block(p, pos + way * (far - 1 - step))
            return sums

        def gather_pair(held):
            if n > LONGEST_RING:
                return [lax.all_gather(x, "rows", axis=0, tiled=True) for x in held]
            full = []
            for x in held:
                empty = jnp.zeros((height * n, x.shape[1]), x.dtype)
                full.append(lax.dynamic_update_slice_in_dim(empty, x, row * height, 0))
            live = {(i, way): x for i, x in enumerate(held) for way in (1, -1)}
            for step in range(n // 2):
                for i in range(len(held)):
                    for way, far in hops_of(i):
                        if step >= far:
                            continue
                        live[i, way] = hop(live[i, way], way)
                        full[i] = lax.dynamic_update_slice_in_dim(
                            full[i], live[i, way], start_of(pos - way * (step + 1)), 0
                        )
            return full

        firsts, seconds, exchanged = [], [], []

        def finish(number, pair, sums):
            updates = []
            for (m, s), projected in zip(pair, sums):
                first, second, update = moment_step(
                    projected, part(moment1, m, s), part(moment2, m, s), scale
                )
                firsts.append(first)
                seconds.append(second)
                updates.append(update)
            for (m, s), full in zip(pair, gather_pair(updates)):
                back = jnp.dot(basis[m], full, preferred_element_type=jnp.float32)
                fresh = part(weights, m, s).astype(jnp.float32) - 0.5 * back
                fresh = fresh.astype(jnp.bfloat16)
                exchanged.append([fresh] + [from_chip(fresh, k) for k in range(1, chips)])

        sums = None
        pairs = [chunks[i : i + 2] for i in range(0, len(chunks), 2)]
        for number, pair in enumerate(pairs):
            held = partials[2 * number : 2 * number + 2]
            if sums is not None:
                held, sums = tie((held, sums))
            sums_before, sums = sums, reduce_pair(held)
            if number >= 1:
                finish(number - 1, pairs[number - 1], sums_before)
                sums, exchanged[-2][0], exchanged[-1][0] = tie(
                    (sums, exchanged[-2][0], exchanged[-1][0])
                )
        finish(len(pairs) - 1, pairs[-1], sums)

        shape = (mats, rows, cols * dp)
        count = len(chunks)
        out = None
        for i, (m, s) in enumerate(chunks):
            pieces = list(exchanged[i])
            if i < count - 2:
                pieces[1:], exchanged[-1][0] = tie((pieces[1:], exchanged[-1][0]))
            if i >= 2:
                pieces[1:], out = tie((pieces[1:], out))
            if cores == 2:
                pieces = pieces + [from_core(x) for x in pieces]
            out = place(groups, pieces, out, shape, m, s)

        def whole(parts):
            return jnp.stack(
                [
                    jnp.concatenate(parts[m * SPLITS : (m + 1) * SPLITS], axis=1)
                    for m in range(mats)
                ]
            )

        return (out, whole(firsts), whole(seconds))

    return jax.shard_map(
        local,
        mesh=mesh,
        in_specs=(
            P(None, "rows", "dp"),
            P(None, "rows", None),
            P(None, "rows", "dp"),
            P(None, "rows", "dp"),
            P(None, "rows", "dp"),
        ),
        out_specs=(P(None, "rows", None), P(None, "rows", "dp"), P(None, "rows", "dp")),
        check_vma=False,
    )
```

```python
import math

import jax
import jax.numpy as jnp
from jax import lax
from jax.experimental import pallas as pl
from jax.experimental.pallas import tpu as pltpu
from jax.sharding import PartitionSpec as P

STEP = 10
SPLITS = 2
LONGEST_RING = 8
CHUNK = 256
VMEM_LIMIT = 31 * 1024 * 1024


def moment_step(projected, moment1, moment2, scale):
    scaled = scale * projected
    first = 0.9 * moment1 + 0.1 * scaled
    second = 0.999 * moment2 + 0.001 * scaled * scaled
    first_bias_correction = 1.0 - 0.9**STEP
    second_fix = 1.0 - 0.999**STEP
    low_rank_update = (
        first / first_bias_correction / (jnp.sqrt(second / second_fix) + 1e-08)
    ).astype(jnp.bfloat16)
    return (first, second, low_rank_update)


def tile_of(width):
    tile = 128
    for cand in range(128, 1025, 128):
        if width % cand == 0:
            tile = cand
    return tile


def place(groups, pieces, out, shape, mat, split):
    count = len(pieces)
    rows, width = pieces[0].shape
    tile = tile_of(width)
    tiles = width // tile

    def piece_spec(p):
        def index(i, j, groups_ref):
            return (0, jnp.where(i == p, j, jnp.where(i < p, 0, tiles - 1)))

        return pl.BlockSpec((rows, tile), index)

    def out_index(i, j, groups_ref):
        return (mat, 0, groups_ref[i] * (SPLITS * tiles) + split * tiles + j)

    def kernel(groups_ref, *refs):
        out_ref = refs[-1]
        for p in range(count):

            @pl.when(pl.program_id(0) == p)
            def _():
                out_ref[0] = refs[p][...]

    extra = [] if out is None else [out]
    return pl.pallas_call(
        kernel,
        grid_spec=pltpu.PrefetchScalarGridSpec(
            num_scalar_prefetch=1,
            grid=(count, tiles),
            in_specs=[piece_spec(p) for p in range(count)]
            + [pl.BlockSpec(memory_space=pl.ANY) for _ in extra],
            out_specs=pl.BlockSpec((1, rows, tile), out_index),
        ),
        out_shape=jax.ShapeDtypeStruct(shape, pieces[0].dtype),
        input_output_aliases={} if out is None else {1 + count: 0},
        cost_estimate=pl.CostEstimate(
            flops=0, bytes_accessed=4 * count * rows * width, transcendentals=0
        ),
        name="place",
    )(groups, *pieces, *extra)


def fused_step(mesh_shape, chunk, grads, basis, moment1, moment2, weights, limit):
    mats, rows, cols = grads.shape
    rank = basis.shape[2]
    height = moment1.shape[1]
    dp = mesh_shape["dp"]
    line = mesh_shape["rows"] // 2
    band = 2 * height
    half = chunk // 2
    per = cols // chunk
    count = mats * per
    hops = line - 1
    ahead = 2
    deep, few, cuts = 8, 4, 4
    back_lag = 2 * line
    ticks = count + back_lag + 3
    f32, bf16 = jnp.float32, jnp.bfloat16

    def kernel(
        grads_ref, basis_ref, first_ref, second_ref, weights_ref,
        out, m1, m2,
        gv, raw, own_b, pair_b, turned, wv,
        part, rup, rdn, proj, upd, sq_out, sq_in, scale_v,
        raw_s, raw_r, bas_s, bas_r, share_s, share_r, load, rs_s, rs_r, proj_s, proj_r,
        upd_s, upd_r, ag_s, ag_r, x_s, x_r, core_s, core_r, fwd_s, fwd_r,
        sq_s, sq_r,
        lead, lead_up, lead_dn, lead_in, lead_s, lead_r, pair_s, pair_r,
    ):
        me, row = lax.axis_index("dp"), lax.axis_index("rows")
        z, y, core = row // 2, row % 2, me % 2
        flip = line - 1 - z
        core_peer = me + 1 - 2 * (me % 2)
        x_peer = (me + 2) % dp
        y_peer = row + 1 - 2 * y
        above = jnp.minimum(z + 1, line - 1) * 2 + y
        below = jnp.maximum(z - 1, 0) * 2 + y

        def remote(src, dst, s, r, device):
            return pltpu.make_async_remote_copy(
                src_ref=src, dst_ref=dst, send_sem=s, recv_sem=r,
                device_id=device, device_id_type=pl.DeviceIdType.MESH,
            )

        def rows_at(b):
            return pl.ds(pl.multiple_of(b * band, band), band)

        def spot(c):
            return c // per, c % per

        def cols_at(j):
            return pl.ds(pl.multiple_of(j * chunk, chunk), chunk)

        def out_at(owner, j):
            return pl.ds(pl.multiple_of(owner * cols + j * chunk, 128), chunk)

        def raw_copy(c):
            m, j = spot(c)
            src = pl.ds(pl.multiple_of(j * chunk + (1 - y) * half, half), half)
            dst = pl.ds(pl.multiple_of(j * half, half), half)
            return remote(
                grads_ref.at[m, :, src], raw.at[m, :, dst],
                raw_s.at[c], raw_r.at[c], (me, y_peer),
            )

        def basis_half(k):
            return pl.ds(pl.multiple_of(k * (rows // 2), rows // 2), rows // 2)

        def basis_copy(m, q):
            size = rows // 2 // cuts
            at = pl.ds(pl.multiple_of(core * (rows // 2) + q * size, size), size)
            return remote(
                basis_ref.at[m, at, :], pair_b.at[m, at, :],
                bas_s.at[m, q], bas_r.at[m, q], (me, y_peer),
            )

        def basis_share(m, k):
            ref = pair_b.at[m, basis_half(k), :]
            return remote(ref, ref, share_s.at[m], share_r.at[m], (core_peer, row))

        def up_block(t):
            return line - 1 - t + z

        def down_block(t):
            return t - line + 1 + z

        def rs_copy(c, t, way, b):
            slot = c % few
            buf, dev = (rup, above) if way == 0 else (rdn, below)
            return remote(
                part.at[c % deep, rows_at(b), :], buf.at[slot, t],
                rs_s.at[way, slot, t], rs_r.at[way, slot, t], (me, dev),
            )

        def rs_sends(c, t, act):
            @pl.when((z <= line - 2) & (z <= t))
            def _():
                act(rs_copy(c, t, 0, up_block(t)))

            @pl.when((z >= 1) & (flip <= t))
            def _():
                act(rs_copy(c, t, 1, down_block(t)))

        def rs_recv(c, t):
            slot = c % few

            @pl.when((z >= 1) & (z <= t))
            def _():
                rs_copy(c, t - 1, 0, z).wait_recv()
                b = rows_at(up_block(t))
                part[c % deep, b, :] = part[c % deep, b, :] + rup[slot, t - 1]

            @pl.when((flip >= 1) & (flip <= t))
            def _():
                rs_copy(c, t - 1, 1, z).wait_recv()
                b = rows_at(down_block(t))
                part[c % deep, b, :] = part[c % deep, b, :] + rdn[slot, t - 1]

        def lead_copy(t, way, b):
            buf, dev = (lead_up, above) if way == 0 else (lead_dn, below)
            return remote(
                lead.at[rows_at(b), :], buf.at[t],
                lead_s.at[way, t], lead_r.at[way, t], (me, dev),
            )

        def lead_sends(t, act):
            @pl.when((z <= line - 2) & (z <= t))
            def _():
                act(lead_copy(t, 0, up_block(t)))

            @pl.when((z >= 1) & (flip <= t))
            def _():
                act(lead_copy(t, 1, down_block(t)))

        def lead_recv(t):
            @pl.when((z >= 1) & (z <= t))
            def _():
                lead_copy(t - 1, 0, z).wait_recv()
                b = rows_at(up_block(t))
                lead[b, :] = lead[b, :] + lead_up[t - 1]

            @pl.when((flip >= 1) & (flip <= t))
            def _():
                lead_copy(t - 1, 1, z).wait_recv()
                b = rows_at(down_block(t))
                lead[b, :] = lead[b, :] + lead_dn[t - 1]

        def lead_pair():
            src = pl.ds(pl.multiple_of(z * band + (1 - y) * height, height), height)
            return remote(
                lead.at[src, :], lead_in, pair_s.at[0], pair_r.at[0], (me, y_peer)
            )

        def proj_copy(c):
            src = pl.ds(pl.multiple_of(z * band + (1 - y) * height, height), height)
            dst = pl.ds(pl.multiple_of(y * half, half), half)
            return remote(
                part.at[c % deep, src, :], proj.at[c % few, :, dst],
                proj_s.at[c % few], proj_r.at[c % few], (me, y_peer),
            )

        def own_rows():
            return pl.ds(pl.multiple_of(row * height, height), height)

        def upd_copy(c):
            ref = upd.at[c % deep, own_rows(), :]
            return remote(ref, ref, upd_s.at[c % few], upd_r.at[c % few], (me, y_peer))

        def ag_copy(c, t, way, b):
            ref = upd.at[c % deep, rows_at(b), :]
            dev = above if way == 0 else below
            return remote(
                ref, ref, ag_s.at[way, c % few, t], ag_r.at[way, c % few, t], (me, dev)
            )

        def ag_sends(c, t, act):
            @pl.when((z <= line - 2) & (z >= t))
            def _():
                act(ag_copy(c, t, 0, z - t))

            @pl.when((z >= 1) & (z + t <= line - 1))
            def _():
                act(ag_copy(c, t, 1, z + t))

        def ag_recv(c, t):
            @pl.when(z >= t + 1)
            def _():
                ag_copy(c, t, 0, z - 1 - t).wait_recv()

            @pl.when(z + 1 + t <= line - 1)
            def _():
                ag_copy(c, t, 1, z + 1 + t).wait_recv()

        def x_copy(c, owner):
            m, j = spot(c)
            ref = out.at[m, :, out_at(owner, j)]
            return remote(ref, ref, x_s.at[c % deep], x_r.at[c % deep], (x_peer, row))

        def core_copy(c, owner):
            m, j = spot(c)
            ref = out.at[m, :, out_at(owner, j)]
            return remote(
                ref, ref, core_s.at[c % deep], core_r.at[c % deep], (core_peer, row)
            )

        def fwd_copy(c, owner):
            m, j = spot(c)
            ref = out.at[m, :, out_at(owner, j)]
            return remote(
                ref, ref, fwd_s.at[c % deep], fwd_r.at[c % deep], (core_peer, row)
            )

        def start(copy):
            copy.start()

        def sent(copy):
            copy.wait_send()

        loads = [
            pltpu.make_async_copy(basis_ref, own_b, load.at[0]),
            pltpu.make_async_copy(first_ref, m1, load.at[1]),
            pltpu.make_async_copy(second_ref, m2, load.at[2]),
            pltpu.make_async_copy(weights_ref, wv, load.at[3]),
        ]
        grad_loads = [
            pltpu.make_async_copy(grads_ref.at[m], gv.at[m], load.at[4 + m])
            for m in range(mats)
        ]
        loads[0].start()
        for copy in grad_loads:
            copy.start()
        for copy in loads[1:]:
            copy.start()

        barrier = pltpu.get_barrier_semaphore()
        peers = [(core_peer, row), (x_peer, row), (me, y_peer)] + [
            (me, ((z + d) % line) * 2 + y) for d in range(1, line)
        ]
        for device in peers:
            pl.semaphore_signal(
                barrier, inc=1, device_id=device, device_id_type=pl.DeviceIdType.MESH
            )
        pl.semaphore_wait(barrier, len(peers))

        for q in range(cuts):
            basis_copy(0, q).start()
        for c in range(1, 1 + ahead):
            raw_copy(c).start()

        def turn(which, ref, m):
            for i in range(0, rows, 128):
                turned[which, m, :, i : i + 128] = ref[m, i : i + 128, :].T

        loads[0].wait()
        turn(0, own_b, 0)
        grad_loads[0].wait()
        lead[...] = jnp.dot(turned[0, 0], gv[0, :, :chunk], preferred_element_type=f32)
        lead_sends(0, start)

        squares = jnp.zeros((16, 128), f32)
        for m in range(mats):
            if m:
                grad_loads[m].wait()

            def square(i, acc, m=m):
                wide = gv[m, pl.ds(pl.multiple_of(i * 16, 16), 16), :].astype(f32)
                wide = wide * wide
                for k in range(0, cols, 128):
                    acc = acc + wide[:, k : k + 128]
                return acc

            squares = lax.fori_loop(0, rows // 16, square, squares)
        sq_out[0] = squares[:8] + squares[8:]

        def sq_copy(k, device, slot):
            return remote(sq_out.at[k], sq_in.at[slot], sq_s.at[slot], sq_r.at[slot], device)

        def sq_line(d):
            return sq_copy(3, (me, ((z + d) % line) * 2 + y), 2 + d)

        sq_copy(0, (core_peer, row), 0).start()
        lead_recv(1)
        lead_sends(1, start)
        for q in range(cuts):
            basis_copy(0, q).wait_recv()
        basis_share(0, core).start()
        for m in range(1, mats):
            turn(0, own_b, m)
        for copy in loads[1:]:
            copy.wait()
        sq_copy(0, (core_peer, row), 0).wait()
        sq_out[1] = sq_out[0] + sq_in[0]
        sq_copy(1, (x_peer, row), 1).start()
        basis_share(0, 1 - core).wait_recv()
        turn(1, pair_b, 0)
        for t in range(2, hops):
            lead_recv(t)
            lead_sends(t, start)

        def tick(now, carry):
            def stage(lag, body, first=0):
                c = now - lag + 1

                @pl.when((c >= first) & (c < count))
                def _():
                    body(c)

            for m in range(1, mats):

                for q in range(cuts):

                    @pl.when(now == max(m * per - 2 * cuts - 4 + 2 * q, 0))
                    def _():
                        basis_copy(m, q).start()

                @pl.when(now == max(m * per - 4, 1))
                def _():
                    for q in range(cuts):
                        basis_copy(m, q).wait_recv()
                    basis_share(m, core).start()

                @pl.when(now == m * per - 1)
                def _():
                    basis_share(m, 1 - core).wait_recv()
                    turn(1, pair_b, m)

            def last(c):
                fwd_copy(c, (core_peer + 2) % dp).wait_recv()
                fwd_copy(c, x_peer).wait_send()
                x_copy(c, me).wait_send()
                core_copy(c, me).wait_send()

            stage(back_lag + 3, last)

            def forward(c):
                x_copy(c, x_peer).wait_recv()
                fwd_copy(c, x_peer).start()
                core_copy(c, core_peer).wait_recv()

            stage(back_lag + 2, forward)

            def back(c):
                m, j = spot(c)
                ag_recv(c, hops - 1)
                product = jnp.dot(own_b[m], upd[c % deep], preferred_element_type=f32)
                fresh = wv[m, :, cols_at(j)].astype(f32) - 0.5 * product
                out[m, :, out_at(me, j)] = fresh.astype(bf16)
                x_copy(c, me).start()
                core_copy(c, me).start()

            stage(back_lag, back)

            for t in range(hops - 1, 0, -1):

                def relay(c, t=t):
                    ag_recv(c, t - 1)
                    ag_sends(c, t, start)

                stage(line + 1 + t, relay)

            def spread(c):
                upd_copy(c).wait_recv()
                ag_sends(c, 0, start)

            stage(line + 1, spread)

            def step(c):
                m, j = spot(c)

                @pl.when(c == 0)
                def _():
                    lead_pair().wait_recv()
                    proj[0] = proj[0] + lead_in[...]

                @pl.when(c > 0)
                def _():
                    proj_copy(c).wait_recv()

                at = cols_at(j)
                first, second, update = moment_step(
                    proj[c % few], m1[m, :, at], m2[m, :, at], scale_v[0:1, 0:1]
                )
                upd[c % deep, own_rows(), :] = update
                upd_copy(c).start()
                m1[m, :, at] = first
                m2[m, :, at] = second

            stage(line, step)

            def complete(c):
                keep = pl.ds(pl.multiple_of(z * band + y * height, height), height)

                @pl.when(c == 0)
                def _():
                    lead_recv(hops)
                    lead_pair().start()
                    proj[0] = lead[keep, :]

                @pl.when(c > 0)
                def _():
                    rs_recv(c, hops)
                    dst = pl.ds(pl.multiple_of(y * half, half), half)
                    proj_copy(c).start()
                    proj[c % few, :, dst] = part[c % deep, keep, :]

            stage(hops, complete)

            for t in range(hops - 1, 0, -1):

                def middle(c, t=t):
                    rs_recv(c, t)
                    rs_sends(c, t, start)

                stage(t, middle, 1)

            def project(c):
                m, j = spot(c)
                raw_copy(c).wait_recv()
                mine = pl.ds(pl.multiple_of(j * chunk + y * half, half), half)
                theirs = pl.ds(pl.multiple_of(j * half, half), half)
                part[c % deep] = jnp.dot(
                    turned[0, m], gv[m, :, mine], preferred_element_type=f32
                ) + jnp.dot(turned[1, m], raw[m, :, theirs], preferred_element_type=f32)
                rs_sends(c, 0, start)

            stage(0, project, 1)

            @pl.when(now + 1 + ahead < count)
            def _():
                raw_copy(now + 1 + ahead).start()

            @pl.when(now == 0)
            def _():
                sq_copy(1, (x_peer, row), 1).wait()
                sq_out[2] = sq_out[1] + sq_in[1]
                sq_copy(2, (me, y_peer), 2).start()

            @pl.when(now == 1)
            def _():
                sq_copy(2, (me, y_peer), 2).wait()
                sq_out[3] = sq_out[2] + sq_in[2]
                for d in range(1, line):
                    sq_line(d).start()

            @pl.when(now == 2)
            def _():
                whole = sq_out[3]
                for d in range(1, line):
                    sq_line(d).wait()
                    whole = whole + sq_in[2 + d]
                total = jnp.sum(whole, axis=(0, 1), keepdims=True)
                scale = limit / jnp.maximum(jnp.sqrt(total), limit)
                scale_v[...] = jnp.broadcast_to(scale, scale_v.shape)

            @pl.when(now == 4)
            def _():
                for t in range(hops):
                    lead_sends(t, sent)
                lead_pair().wait_send()

            for t in range(hops):

                def freed(c, t=t):
                    rs_sends(c, t, sent)

                stage(t + 2, freed, 1)

                def freed_update(c, t=t):
                    ag_sends(c, t, sent)

                stage(line + 3 + t, freed_update)

            def freed_pair(c):
                raw_copy(c).wait_send()
                proj_copy(c).wait_send()

            stage(hops + 2, freed_pair, 1)

            def freed_own(c):
                upd_copy(c).wait_send()

            stage(line + 2, freed_own)
            return carry

        lax.fori_loop(0, ticks, tick, 0)
        for m in range(mats):
            for q in range(cuts):
                basis_copy(m, q).wait_send()
            basis_share(m, core).wait_send()

    dma = pltpu.SemaphoreType.DMA
    anywhere = pl.BlockSpec(memory_space=pl.ANY)
    fresh, first, second = pl.pallas_call(
        kernel,
        out_shape=(
            pltpu.VMEM((mats, rows, cols * dp), bf16),
            pltpu.VMEM(moment1.shape, f32),
            pltpu.VMEM(moment2.shape, f32),
        ),
        in_specs=[anywhere] * 5,
        out_specs=(pl.BlockSpec(memory_space=pltpu.VMEM),) * 3,
        scratch_shapes=[
            pltpu.VMEM((mats, rows, cols), bf16),
            pltpu.VMEM((mats, rows, cols // 2), bf16),
            pltpu.VMEM((mats, rows, rank), bf16),
            pltpu.VMEM((mats, rows, rank), bf16),
            pltpu.VMEM((2, mats, rank, rows), bf16),
            pltpu.VMEM((mats, rows, cols), bf16),
            pltpu.VMEM((deep, rank, half), f32),
            pltpu.VMEM((few, hops, band, half), f32),
            pltpu.VMEM((few, hops, band, half), f32),
            pltpu.VMEM((few, height, chunk), f32),
            pltpu.VMEM((deep, rank, chunk), bf16),
            pltpu.VMEM((4, 8, 128), f32),
            pltpu.VMEM((2 + line, 8, 128), f32),
            pltpu.VMEM((8, 128), f32),
            dma((count,)), dma((count,)), dma((mats, cuts)), dma((mats, cuts)),
            dma((mats,)), dma((mats,)), dma((4 + mats,)),
            dma((2, few, hops)), dma((2, few, hops)), dma((few,)), dma((few,)),
            dma((few,)), dma((few,)), dma((2, few, hops)), dma((2, few, hops)),
            dma((deep,)), dma((deep,)), dma((deep,)), dma((deep,)),
            dma((deep,)), dma((deep,)), dma((2 + line,)), dma((2 + line,)),
            pltpu.VMEM((rank, chunk), f32),
            pltpu.VMEM((hops, band, chunk), f32),
            pltpu.VMEM((hops, band, chunk), f32),
            pltpu.VMEM((height, chunk), f32),
            dma((2, hops)), dma((2, hops)), dma((1,)), dma((1,)),
        ],
        compiler_params=pltpu.CompilerParams(
            collective_id=0, has_side_effects=True, vmem_limit_bytes=VMEM_LIMIT
        ),
        cost_estimate=pl.CostEstimate(
            flops=6 * mats * rows * rank * cols,
            bytes_accessed=8 * mats * rows * cols,
            transcendentals=0,
        ),
        name="step",
    )(grads, basis, moment1, moment2, weights)
    (fresh,) = settle((fresh,), 4)
    return (fresh, *settle((first, second), 1))


def settle(arrays, cuts):
    count = len(arrays)

    def kernel(*refs):
        done = refs[-1]
        copies = []
        for i in range(count):
            size = arrays[i].shape[1] // cuts
            for m in range(arrays[i].shape[0]):
                for k in range(cuts):
                    at = pl.ds(k * size, size)
                    copies.append(
                        pltpu.make_async_copy(
                            refs[i].at[m, at, :],
                            refs[count + i].at[m, at, :],
                            done.at[len(copies)],
                        )
                    )
        for copy in copies:
            copy.start()
        for copy in copies:
            copy.wait()

    return pl.pallas_call(
        kernel,
        out_shape=tuple(jax.ShapeDtypeStruct(x.shape, x.dtype) for x in arrays),
        in_specs=[pl.BlockSpec(memory_space=pltpu.VMEM)] * count,
        out_specs=(pl.BlockSpec(memory_space=pl.ANY),) * count,
        scratch_shapes=[
            pltpu.SemaphoreType.DMA((cuts * sum(x.shape[0] for x in arrays),))
        ],
        compiler_params=pltpu.CompilerParams(vmem_limit_bytes=1024 * 1024),
        name="settle",
    )(*arrays)


def solution(mesh):
    dp = mesh.shape["dp"]
    cores = 2 if dp % 2 == 0 else 1
    chips = dp // cores
    n = mesh.shape["rows"]
    ring = [2 * q if q < n // 2 else 2 * (n - 1 - q) + 1 for q in range(n)]

    def sum_all(x):
        if dp & (dp - 1) or n & (n - 1):
            return lax.psum(x, ("dp", "rows"))
        x = jnp.full((8, 128), x, jnp.float32)
        for axis, size in (("rows", n), ("dp", dp)):
            bit = 1
            while bit < size:
                x = x + lax.ppermute(x, axis, [(i, i ^ bit) for i in range(size)])
                bit *= 2
        return x[0, 0]

    def local(grads, basis, moment1, moment2, weights):
        mats, rows, cols = grads.shape
        width = cols // SPLITS
        limit = 1.0 * math.sqrt(mats * rows * mesh.shape["rows"] * cols * dp)
        if dp == 4 and n == LONGEST_RING and cols % CHUNK == 0:
            return fused_step(
                mesh.shape, CHUNK, grads, basis, moment1, moment2, weights, limit
            )

        chunks = [(m, s) for m in range(mats) for s in range(SPLITS)]

        def part(x, m, s):
            return x[m, :, s * width : (s + 1) * width]

        partials = [
            lax.dot_general(
                basis[m],
                part(grads, m, s),
                (((0,), (0,)), ((), ())),
                preferred_element_type=jnp.float32,
            )
            for m, s in chunks
        ]
        wide = grads.astype(jnp.float32)
        total = sum_all(jnp.sum(wide * wide))
        scale = limit / jnp.maximum(jnp.sqrt(total), limit)

        me = lax.axis_index("dp")
        chip, core = me // cores, me % cores
        order = [(k, c) for c in range(cores) for k in range(chips)]
        groups = jnp.stack(
            [((chip + chips - k) % chips) * cores + (core + c) % cores for k, c in order]
        ).astype(jnp.int32)

        def from_chip(x, k):
            pairs = [
                (a * cores + c, ((a + k) % chips) * cores + c)
                for a in range(chips)
                for c in range(cores)
            ]
            return lax.ppermute(x, "dp", pairs)

        def from_core(x):
            pairs = [
                (a * cores + c, a * cores + (c + 1) % cores)
                for a in range(chips)
                for c in range(cores)
            ]
            return lax.ppermute(x, "dp", pairs)

        tie = lax.optimization_barrier
        row = lax.axis_index("rows")
        pos = jnp.where(row % 2 == 0, row // 2, n - 1 - row // 2)
        height = moment1.shape[1]

        def start_of(q):
            q = (q + 2 * n) % n
            return jnp.where(q < n // 2, 2 * q, 2 * (n - 1 - q) + 1) * height

        def hop(x, way):
            return lax.ppermute(
                x, "rows", [(ring[q], ring[(q + way) % n]) for q in range(n)]
            )

        def block(partial, q):
            return lax.dynamic_slice_in_dim(partial, start_of(q), height, 0)

        def hops_of(i):
            near, far = (n - 1) // 2, n // 2
            return ((1, far), (-1, near)) if i % 2 == 0 else ((1, near), (-1, far))

        def reduce_pair(held):
            if n > LONGEST_RING:
                return [
                    lax.psum_scatter(p, "rows", scatter_dimension=0, tiled=True)
                    for p in held
                ]
            sums = [block(p, pos) for p in held]
            live = {}
            for i, p in enumerate(held):
                for way, far in hops_of(i):
                    if far:
                        live[i, way] = block(p, pos + way * far)
            for step in range(n // 2):
                for i, p in enumerate(held):
                    for way, far in hops_of(i):
                        if step >= far:
                            continue
                        got = hop(live[i, way], way)
                        if step == far - 1:
                            sums[i] = sums[i] + got
                        else:
                            live[i, way] = got + block(p, pos + way * (far - 1 - step))
            return sums

        def gather_pair(held):
            if n > LONGEST_RING:
                return [lax.all_gather(x, "rows", axis=0, tiled=True) for x in held]
            full = []
            for x in held:
                empty = jnp.zeros((height * n, x.shape[1]), x.dtype)
                full.append(lax.dynamic_update_slice_in_dim(empty, x, row * height, 0))
            live = {(i, way): x for i, x in enumerate(held) for way in (1, -1)}
            for step in range(n // 2):
                for i in range(len(held)):
                    for way, far in hops_of(i):
                        if step >= far:
                            continue
                        live[i, way] = hop(live[i, way], way)
                        full[i] = lax.dynamic_update_slice_in_dim(
                            full[i], live[i, way], start_of(pos - way * (step + 1)), 0
                        )
            return full

        firsts, seconds, exchanged = [], [], []

        def finish(number, pair, sums):
            updates = []
            for (m, s), projected in zip(pair, sums):
                first, second, update = moment_step(
                    projected, part(moment1, m, s), part(moment2, m, s), scale
                )
                firsts.append(first)
                seconds.append(second)
                updates.append(update)
            for (m, s), full in zip(pair, gather_pair(updates)):
                back = jnp.dot(basis[m], full, preferred_element_type=jnp.float32)
                fresh = part(weights, m, s).astype(jnp.float32) - 0.5 * back
                fresh = fresh.astype(jnp.bfloat16)
                exchanged.append([fresh] + [from_chip(fresh, k) for k in range(1, chips)])

        sums = None
        pairs = [chunks[i : i + 2] for i in range(0, len(chunks), 2)]
        for number, pair in enumerate(pairs):
            held = partials[2 * number : 2 * number + 2]
            if sums is not None:
                held, sums = tie((held, sums))
            sums_before, sums = sums, reduce_pair(held)
            if number >= 1:
                finish(number - 1, pairs[number - 1], sums_before)
                sums, exchanged[-2][0], exchanged[-1][0] = tie(
                    (sums, exchanged[-2][0], exchanged[-1][0])
                )
        finish(len(pairs) - 1, pairs[-1], sums)

        shape = (mats, rows, cols * dp)
        count = len(chunks)
        out = None
        for i, (m, s) in enumerate(chunks):
            pieces = list(exchanged[i])
            if i < count - 2:
                pieces[1:], exchanged[-1][0] = tie((pieces[1:], exchanged[-1][0]))
            if i >= 2:
                pieces[1:], out = tie((pieces[1:], out))
            if cores == 2:
                pieces = pieces + [from_core(x) for x in pieces]
            out = place(groups, pieces, out, shape, m, s)

        def whole(parts):
            return jnp.stack(
                [
                    jnp.concatenate(parts[m * SPLITS : (m + 1) * SPLITS], axis=1)
                    for m in range(mats)
                ]
            )

        return (out, whole(firsts), whole(seconds))

    return jax.shard_map(
        local,
        mesh=mesh,
        in_specs=(
            P(None, "rows", "dp"),
            P(None, "rows", None),
            P(None, "rows", "dp"),
            P(None, "rows", "dp"),
            P(None, "rows", "dp"),
        ),
        out_specs=(P(None, "rows", None), P(None, "rows", "dp"), P(None, "rows", "dp")),
        check_vma=False,
    )
```

```python
import math

import jax
import jax.numpy as jnp
from jax import lax
from jax.experimental import pallas as pl
from jax.experimental.pallas import tpu as pltpu
from jax.sharding import PartitionSpec as P

STEP = 10
SPLITS = 2
LONGEST_RING = 8
CHUNK = 256
VMEM_LIMIT = 31 * 1024 * 1024


def moment_step(projected, moment1, moment2, scale):
    scaled = scale * projected
    first = 0.9 * moment1 + 0.1 * scaled
    second = 0.999 * moment2 + 0.001 * scaled * scaled
    first_bias_correction = 1.0 - 0.9**STEP
    second_fix = 1.0 - 0.999**STEP
    low_rank_update = (
        first / first_bias_correction / (jnp.sqrt(second / second_fix) + 1e-08)
    ).astype(jnp.bfloat16)
    return (first, second, low_rank_update)


def tile_of(width):
    tile = 128
    for cand in range(128, 1025, 128):
        if width % cand == 0:
            tile = cand
    return tile


def place(groups, pieces, out, shape, mat, split):
    count = len(pieces)
    rows, width = pieces[0].shape
    tile = tile_of(width)
    tiles = width // tile

    def piece_spec(p):
        def index(i, j, groups_ref):
            return (0, jnp.where(i == p, j, jnp.where(i < p, 0, tiles - 1)))

        return pl.BlockSpec((rows, tile), index)

    def out_index(i, j, groups_ref):
        return (mat, 0, groups_ref[i] * (SPLITS * tiles) + split * tiles + j)

    def kernel(groups_ref, *refs):
        out_ref = refs[-1]
        for p in range(count):

            @pl.when(pl.program_id(0) == p)
            def _():
                out_ref[0] = refs[p][...]

    extra = [] if out is None else [out]
    return pl.pallas_call(
        kernel,
        grid_spec=pltpu.PrefetchScalarGridSpec(
            num_scalar_prefetch=1,
            grid=(count, tiles),
            in_specs=[piece_spec(p) for p in range(count)]
            + [pl.BlockSpec(memory_space=pl.ANY) for _ in extra],
            out_specs=pl.BlockSpec((1, rows, tile), out_index),
        ),
        out_shape=jax.ShapeDtypeStruct(shape, pieces[0].dtype),
        input_output_aliases={} if out is None else {1 + count: 0},
        cost_estimate=pl.CostEstimate(
            flops=0, bytes_accessed=4 * count * rows * width, transcendentals=0
        ),
        name="place",
    )(groups, *pieces, *extra)


def fused_step(mesh_shape, chunk, grads, basis, moment1, moment2, weights, limit):
    mats, rows, cols = grads.shape
    rank = basis.shape[2]
    height = moment1.shape[1]
    dp = mesh_shape["dp"]
    line = mesh_shape["rows"] // 2
    band = 2 * height
    half = chunk // 2
    per = cols // chunk
    count = mats * per
    hops = line - 1
    ahead = 2
    deep, few, cuts = 8, 4, 4
    back_lag = 2 * line
    ticks = count + back_lag + 3
    f32, bf16 = jnp.float32, jnp.bfloat16

    def kernel(
        grads_ref, basis_ref, first_ref, second_ref, weights_ref,
        out, m1, m2,
        gv, raw, own_b, pair_b, turned, wv,
        part, rup, rdn, proj, upd, sq_out, sq_in, scale_v,
        raw_s, raw_r, bas_s, bas_r, share_s, share_r, load, rs_s, rs_r, proj_s, proj_r,
        upd_s, upd_r, ag_s, ag_r, x_s, x_r, core_s, core_r, fwd_s, fwd_r,
        sq_s, sq_r,
        lead, lead_up, lead_dn, lead_in, lead_s, lead_r, pair_s, pair_r,
    ):
        me, row = lax.axis_index("dp"), lax.axis_index("rows")
        z, y, core = row // 2, row % 2, me % 2
        flip = line - 1 - z
        core_peer = me + 1 - 2 * (me % 2)
        x_peer = (me + 2) % dp
        y_peer = row + 1 - 2 * y
        above = jnp.minimum(z + 1, line - 1) * 2 + y
        below = jnp.maximum(z - 1, 0) * 2 + y

        def remote(src, dst, s, r, device):
            return pltpu.make_async_remote_copy(
                src_ref=src, dst_ref=dst, send_sem=s, recv_sem=r,
                device_id=device, device_id_type=pl.DeviceIdType.MESH,
            )

        def rows_at(b):
            return pl.ds(pl.multiple_of(b * band, band), band)

        def spot(c):
            return c // per, c % per

        def cols_at(j):
            return pl.ds(pl.multiple_of(j * chunk, chunk), chunk)

        def out_at(owner, j):
            return pl.ds(pl.multiple_of(owner * cols + j * chunk, 128), chunk)

        def raw_copy(c):
            m, j = spot(c)
            src = pl.ds(pl.multiple_of(j * chunk + (1 - y) * half, half), half)
            dst = pl.ds(pl.multiple_of(j * half, half), half)
            return remote(
                grads_ref.at[m, :, src], raw.at[m, :, dst],
                raw_s.at[c], raw_r.at[c], (me, y_peer),
            )

        def basis_half(k):
            return pl.ds(pl.multiple_of(k * (rows // 2), rows // 2), rows // 2)

        def basis_copy(m, q):
            size = rows // 2 // cuts
            at = pl.ds(pl.multiple_of(core * (rows // 2) + q * size, size), size)
            return remote(
                basis_ref.at[m, at, :], pair_b.at[m, at, :],
                bas_s.at[m, q], bas_r.at[m, q], (me, y_peer),
            )

        def basis_share(m, k):
            ref = pair_b.at[m, basis_half(k), :]
            return remote(ref, ref, share_s.at[m], share_r.at[m], (core_peer, row))

        def up_block(t):
            return line - 1 - t + z

        def down_block(t):
            return t - line + 1 + z

        def rs_copy(c, t, way, b):
            slot = c % few
            buf, dev = (rup, above) if way == 0 else (rdn, below)
            return remote(
                part.at[c % deep, rows_at(b), :], buf.at[slot, t],
                rs_s.at[way, slot, t], rs_r.at[way, slot, t], (me, dev),
            )

        def rs_sends(c, t, act):
            @pl.when((z <= line - 2) & (z <= t))
            def _():
                act(rs_copy(c, t, 0, up_block(t)))

            @pl.when((z >= 1) & (flip <= t))
            def _():
                act(rs_copy(c, t, 1, down_block(t)))

        def rs_recv(c, t):
            slot = c % few

            @pl.when((z >= 1) & (z <= t))
            def _():
                rs_copy(c, t - 1, 0, z).wait_recv()
                b = rows_at(up_block(t))
                part[c % deep, b, :] = part[c % deep, b, :] + rup[slot, t - 1]

            @pl.when((flip >= 1) & (flip <= t))
            def _():
                rs_copy(c, t - 1, 1, z).wait_recv()
                b = rows_at(down_block(t))
                part[c % deep, b, :] = part[c % deep, b, :] + rdn[slot, t - 1]

        def lead_copy(t, way, b):
            buf, dev = (lead_up, above) if way == 0 else (lead_dn, below)
            return remote(
                lead.at[rows_at(b), :], buf.at[t],
                lead_s.at[way, t], lead_r.at[way, t], (me, dev),
            )

        def lead_sends(t, act):
            @pl.when((z <= line - 2) & (z <= t))
            def _():
                act(lead_copy(t, 0, up_block(t)))

            @pl.when((z >= 1) & (flip <= t))
            def _():
                act(lead_copy(t, 1, down_block(t)))

        def lead_recv(t):
            @pl.when((z >= 1) & (z <= t))
            def _():
                lead_copy(t - 1, 0, z).wait_recv()
                b = rows_at(up_block(t))
                lead[b, :] = lead[b, :] + lead_up[t - 1]

            @pl.when((flip >= 1) & (flip <= t))
            def _():
                lead_copy(t - 1, 1, z).wait_recv()
                b = rows_at(down_block(t))
                lead[b, :] = lead[b, :] + lead_dn[t - 1]

        def lead_pair():
            src = pl.ds(pl.multiple_of(z * band + (1 - y) * height, height), height)
            return remote(
                lead.at[src, :], lead_in, pair_s.at[0], pair_r.at[0], (me, y_peer)
            )

        def proj_copy(c):
            src = pl.ds(pl.multiple_of(z * band + (1 - y) * height, height), height)
            dst = pl.ds(pl.multiple_of(y * half, half), half)
            return remote(
                part.at[c % deep, src, :], proj.at[c % few, :, dst],
                proj_s.at[c % few], proj_r.at[c % few], (me, y_peer),
            )

        def own_rows():
            return pl.ds(pl.multiple_of(row * height, height), height)

        def upd_copy(c):
            ref = upd.at[c % deep, own_rows(), :]
            return remote(ref, ref, upd_s.at[c % few], upd_r.at[c % few], (me, y_peer))

        def ag_copy(c, t, way, b):
            ref = upd.at[c % deep, rows_at(b), :]
            dev = above if way == 0 else below
            return remote(
                ref, ref, ag_s.at[way, c % few, t], ag_r.at[way, c % few, t], (me, dev)
            )

        def ag_sends(c, t, act):
            @pl.when((z <= line - 2) & (z >= t))
            def _():
                act(ag_copy(c, t, 0, z - t))

            @pl.when((z >= 1) & (z + t <= line - 1))
            def _():
                act(ag_copy(c, t, 1, z + t))

        def ag_recv(c, t):
            @pl.when(z >= t + 1)
            def _():
                ag_copy(c, t, 0, z - 1 - t).wait_recv()

            @pl.when(z + 1 + t <= line - 1)
            def _():
                ag_copy(c, t, 1, z + 1 + t).wait_recv()

        def x_copy(c, owner, k):
            m, j = spot(c)
            ref = out.at[m, pl.ds(k * (rows // 2), rows // 2), out_at(owner, j)]
            return remote(
                ref, ref, x_s.at[c % deep, k], x_r.at[c % deep, k], (x_peer, row)
            )

        def core_copy(c, owner):
            m, j = spot(c)
            ref = out.at[m, :, out_at(owner, j)]
            return remote(
                ref, ref, core_s.at[c % deep], core_r.at[c % deep], (core_peer, row)
            )

        def fwd_copy(c, owner):
            m, j = spot(c)
            ref = out.at[m, :, out_at(owner, j)]
            return remote(
                ref, ref, fwd_s.at[c % deep], fwd_r.at[c % deep], (core_peer, row)
            )

        def start(copy):
            copy.start()

        def sent(copy):
            copy.wait_send()

        loads = [
            pltpu.make_async_copy(basis_ref, own_b, load.at[0]),
            pltpu.make_async_copy(first_ref, m1, load.at[1]),
            pltpu.make_async_copy(second_ref, m2, load.at[2]),
            pltpu.make_async_copy(weights_ref, wv, load.at[3]),
        ]
        grad_loads = [
            pltpu.make_async_copy(grads_ref.at[m], gv.at[m], load.at[4 + m])
            for m in range(mats)
        ]
        loads[0].start()
        for copy in grad_loads:
            copy.start()
        for copy in loads[1:]:
            copy.start()

        barrier = pltpu.get_barrier_semaphore()
        peers = [(core_peer, row), (x_peer, row), (me, y_peer)] + [
            (me, ((z + d) % line) * 2 + y) for d in range(1, line)
        ]
        for device in peers:
            pl.semaphore_signal(
                barrier, inc=1, device_id=device, device_id_type=pl.DeviceIdType.MESH
            )
        pl.semaphore_wait(barrier, len(peers))

        for q in range(cuts):
            basis_copy(0, q).start()
        for c in range(1, 1 + ahead):
            raw_copy(c).start()

        def turn(which, ref, m):
            for i in range(0, rows, 128):
                turned[which, m, :, i : i + 128] = ref[m, i : i + 128, :].T

        loads[0].wait()
        turn(0, own_b, 0)
        grad_loads[0].wait()
        lead[...] = jnp.dot(turned[0, 0], gv[0, :, :chunk], preferred_element_type=f32)
        lead_sends(0, start)

        squares = jnp.zeros((16, 128), f32)
        for m in range(mats):
            if m:
                grad_loads[m].wait()

            def square(i, acc, m=m):
                wide = gv[m, pl.ds(pl.multiple_of(i * 16, 16), 16), :].astype(f32)
                wide = wide * wide
                for k in range(0, cols, 128):
                    acc = acc + wide[:, k : k + 128]
                return acc

            squares = lax.fori_loop(0, rows // 16, square, squares)
        sq_out[0] = squares[:8] + squares[8:]

        def sq_copy(k, device, slot):
            return remote(sq_out.at[k], sq_in.at[slot], sq_s.at[slot], sq_r.at[slot], device)

        def sq_line(d):
            return sq_copy(3, (me, ((z + d) % line) * 2 + y), 2 + d)

        sq_copy(0, (core_peer, row), 0).start()
        lead_recv(1)
        lead_sends(1, start)
        for q in range(cuts):
            basis_copy(0, q).wait_recv()
        basis_share(0, core).start()
        for m in range(1, mats):
            turn(0, own_b, m)
        for copy in loads[1:]:
            copy.wait()
        sq_copy(0, (core_peer, row), 0).wait()
        sq_out[1] = sq_out[0] + sq_in[0]
        sq_copy(1, (x_peer, row), 1).start()
        basis_share(0, 1 - core).wait_recv()
        turn(1, pair_b, 0)
        for t in range(2, hops):
            lead_recv(t)
            lead_sends(t, start)

        def tick(now, carry):
            def stage(lag, body, first=0):
                c = now - lag + 1

                @pl.when((c >= first) & (c < count))
                def _():
                    body(c)

            for m in range(1, mats):

                for q in range(cuts):

                    @pl.when(now == max(m * per - 2 * cuts - 4 + 2 * q, 0))
                    def _():
                        basis_copy(m, q).start()

                @pl.when(now == max(m * per - 4, 1))
                def _():
                    for q in range(cuts):
                        basis_copy(m, q).wait_recv()
                    basis_share(m, core).start()

                @pl.when(now == m * per - 1)
                def _():
                    basis_share(m, 1 - core).wait_recv()
                    turn(1, pair_b, m)

            def last(c):
                fwd_copy(c, (core_peer + 2) % dp).wait_recv()
                fwd_copy(c, x_peer).wait_send()
                for k in range(2):
                    x_copy(c, me, k).wait_send()
                core_copy(c, me).wait_send()

            stage(back_lag + 3, last)

            def forward(c):
                for k in range(2):
                    x_copy(c, x_peer, k).wait_recv()
                fwd_copy(c, x_peer).start()
                core_copy(c, core_peer).wait_recv()

            stage(back_lag + 2, forward)

            def back(c):
                m, j = spot(c)
                ag_recv(c, hops - 1)
                for k in range(2):
                    at = slice(k * (rows // 2), (k + 1) * (rows // 2))
                    product = jnp.dot(
                        own_b[m, at, :], upd[c % deep], preferred_element_type=f32
                    )
                    fresh = wv[m, at, cols_at(j)].astype(f32) - 0.5 * product
                    out[m, at, out_at(me, j)] = fresh.astype(bf16)
                    x_copy(c, me, k).start()
                core_copy(c, me).start()

            stage(back_lag, back)

            for t in range(hops - 1, 0, -1):

                def relay(c, t=t):
                    ag_recv(c, t - 1)
                    ag_sends(c, t, start)

                stage(line + 1 + t, relay)

            def spread(c):
                upd_copy(c).wait_recv()
                ag_sends(c, 0, start)

            stage(line + 1, spread)

            def step(c):
                m, j = spot(c)

                @pl.when(c == 0)
                def _():
                    lead_pair().wait_recv()
                    proj[0] = proj[0] + lead_in[...]

                @pl.when(c > 0)
                def _():
                    proj_copy(c).wait_recv()

                at = cols_at(j)
                first, second, update = moment_step(
                    proj[c % few], m1[m, :, at], m2[m, :, at], scale_v[0:1, 0:1]
                )
                upd[c % deep, own_rows(), :] = update
                upd_copy(c).start()
                m1[m, :, at] = first
                m2[m, :, at] = second

            stage(line, step)

            def complete(c):
                keep = pl.ds(pl.multiple_of(z * band + y * height, height), height)

                @pl.when(c == 0)
                def _():
                    lead_recv(hops)
                    lead_pair().start()
                    proj[0] = lead[keep, :]

                @pl.when(c > 0)
                def _():
                    rs_recv(c, hops)
                    dst = pl.ds(pl.multiple_of(y * half, half), half)
                    proj_copy(c).start()
                    proj[c % few, :, dst] = part[c % deep, keep, :]

            stage(hops, complete)

            for t in range(hops - 1, 0, -1):

                def middle(c, t=t):
                    rs_recv(c, t)
                    rs_sends(c, t, start)

                stage(t, middle, 1)

            @pl.when(now + 1 + ahead < count)
            def _():
                raw_copy(now + 1 + ahead).start()

            def project(c):
                m, j = spot(c)
                raw_copy(c).wait_recv()
                mine = pl.ds(pl.multiple_of(j * chunk + y * half, half), half)
                theirs = pl.ds(pl.multiple_of(j * half, half), half)
                part[c % deep] = jnp.dot(
                    turned[0, m], gv[m, :, mine], preferred_element_type=f32
                ) + jnp.dot(turned[1, m], raw[m, :, theirs], preferred_element_type=f32)
                rs_sends(c, 0, start)

            stage(0, project, 1)

            @pl.when(now == 0)
            def _():
                sq_copy(1, (x_peer, row), 1).wait()
                sq_out[2] = sq_out[1] + sq_in[1]
                sq_copy(2, (me, y_peer), 2).start()

            @pl.when(now == 1)
            def _():
                sq_copy(2, (me, y_peer), 2).wait()
                sq_out[3] = sq_out[2] + sq_in[2]
                for d in range(1, line):
                    sq_line(d).start()

            @pl.when(now == 2)
            def _():
                whole = sq_out[3]
                for d in range(1, line):
                    sq_line(d).wait()
                    whole = whole + sq_in[2 + d]
                total = jnp.sum(whole, axis=(0, 1), keepdims=True)
                scale = limit / jnp.maximum(jnp.sqrt(total), limit)
                scale_v[...] = jnp.broadcast_to(scale, scale_v.shape)

            @pl.when(now == 4)
            def _():
                for t in range(hops):
                    lead_sends(t, sent)
                lead_pair().wait_send()

            for t in range(hops):

                def freed(c, t=t):
                    rs_sends(c, t, sent)

                stage(t + 2, freed, 1)

                def freed_update(c, t=t):
                    ag_sends(c, t, sent)

                stage(line + 3 + t, freed_update)

            def freed_pair(c):
                raw_copy(c).wait_send()
                proj_copy(c).wait_send()

            stage(hops + 2, freed_pair, 1)

            def freed_own(c):
                upd_copy(c).wait_send()

            stage(line + 2, freed_own)
            return carry

        lax.fori_loop(0, ticks, tick, 0)
        for m in range(mats):
            for q in range(cuts):
                basis_copy(m, q).wait_send()
            basis_share(m, core).wait_send()

    dma = pltpu.SemaphoreType.DMA
    anywhere = pl.BlockSpec(memory_space=pl.ANY)
    fresh, first, second = pl.pallas_call(
        kernel,
        out_shape=(
            pltpu.VMEM((mats, rows, cols * dp), bf16),
            pltpu.VMEM(moment1.shape, f32),
            pltpu.VMEM(moment2.shape, f32),
        ),
        in_specs=[anywhere] * 5,
        out_specs=(pl.BlockSpec(memory_space=pltpu.VMEM),) * 3,
        scratch_shapes=[
            pltpu.VMEM((mats, rows, cols), bf16),
            pltpu.VMEM((mats, rows, cols // 2), bf16),
            pltpu.VMEM((mats, rows, rank), bf16),
            pltpu.VMEM((mats, rows, rank), bf16),
            pltpu.VMEM((2, mats, rank, rows), bf16),
            pltpu.VMEM((mats, rows, cols), bf16),
            pltpu.VMEM((deep, rank, half), f32),
            pltpu.VMEM((few, hops, band, half), f32),
            pltpu.VMEM((few, hops, band, half), f32),
            pltpu.VMEM((few, height, chunk), f32),
            pltpu.VMEM((deep, rank, chunk), bf16),
            pltpu.VMEM((4, 8, 128), f32),
            pltpu.VMEM((2 + line, 8, 128), f32),
            pltpu.VMEM((8, 128), f32),
            dma((count,)), dma((count,)), dma((mats, cuts)), dma((mats, cuts)),
            dma((mats,)), dma((mats,)), dma((4 + mats,)),
            dma((2, few, hops)), dma((2, few, hops)), dma((few,)), dma((few,)),
            dma((few,)), dma((few,)), dma((2, few, hops)), dma((2, few, hops)),
            dma((deep, 2)), dma((deep, 2)), dma((deep,)), dma((deep,)),
            dma((deep,)), dma((deep,)), dma((2 + line,)), dma((2 + line,)),
            pltpu.VMEM((rank, chunk), f32),
            pltpu.VMEM((hops, band, chunk), f32),
            pltpu.VMEM((hops, band, chunk), f32),
            pltpu.VMEM((height, chunk), f32),
            dma((2, hops)), dma((2, hops)), dma((1,)), dma((1,)),
        ],
        compiler_params=pltpu.CompilerParams(
            collective_id=0, has_side_effects=True, vmem_limit_bytes=VMEM_LIMIT
        ),
        cost_estimate=pl.CostEstimate(
            flops=6 * mats * rows * rank * cols,
            bytes_accessed=8 * mats * rows * cols,
            transcendentals=0,
        ),
        name="step",
    )(grads, basis, moment1, moment2, weights)
    (fresh,) = settle((fresh,), 4)
    return (fresh, *settle((first, second), 1))


def settle(arrays, cuts):
    count = len(arrays)

    def kernel(*refs):
        done = refs[-1]
        copies = []
        for i in range(count):
            size = arrays[i].shape[1] // cuts
            for m in range(arrays[i].shape[0]):
                for k in range(cuts):
                    at = pl.ds(k * size, size)
                    copies.append(
                        pltpu.make_async_copy(
                            refs[i].at[m, at, :],
                            refs[count + i].at[m, at, :],
                            done.at[len(copies)],
                        )
                    )
        for copy in copies:
            copy.start()
        for copy in copies:
            copy.wait()

    return pl.pallas_call(
        kernel,
        out_shape=tuple(jax.ShapeDtypeStruct(x.shape, x.dtype) for x in arrays),
        in_specs=[pl.BlockSpec(memory_space=pltpu.VMEM)] * count,
        out_specs=(pl.BlockSpec(memory_space=pl.ANY),) * count,
        scratch_shapes=[
            pltpu.SemaphoreType.DMA((cuts * sum(x.shape[0] for x in arrays),))
        ],
        compiler_params=pltpu.CompilerParams(vmem_limit_bytes=1024 * 1024),
        name="settle",
    )(*arrays)


def solution(mesh):
    dp = mesh.shape["dp"]
    cores = 2 if dp % 2 == 0 else 1
    chips = dp // cores
    n = mesh.shape["rows"]
    ring = [2 * q if q < n // 2 else 2 * (n - 1 - q) + 1 for q in range(n)]

    def sum_all(x):
        if dp & (dp - 1) or n & (n - 1):
            return lax.psum(x, ("dp", "rows"))
        x = jnp.full((8, 128), x, jnp.float32)
        for axis, size in (("rows", n), ("dp", dp)):
            bit = 1
            while bit < size:
                x = x + lax.ppermute(x, axis, [(i, i ^ bit) for i in range(size)])
                bit *= 2
        return x[0, 0]

    def local(grads, basis, moment1, moment2, weights):
        mats, rows, cols = grads.shape
        width = cols // SPLITS
        limit = 1.0 * math.sqrt(mats * rows * mesh.shape["rows"] * cols * dp)
        if dp == 4 and n == LONGEST_RING and cols % CHUNK == 0:
            return fused_step(
                mesh.shape, CHUNK, grads, basis, moment1, moment2, weights, limit
            )

        chunks = [(m, s) for m in range(mats) for s in range(SPLITS)]

        def part(x, m, s):
            return x[m, :, s * width : (s + 1) * width]

        partials = [
            lax.dot_general(
                basis[m],
                part(grads, m, s),
                (((0,), (0,)), ((), ())),
                preferred_element_type=jnp.float32,
            )
            for m, s in chunks
        ]
        wide = grads.astype(jnp.float32)
        total = sum_all(jnp.sum(wide * wide))
        scale = limit / jnp.maximum(jnp.sqrt(total), limit)

        me = lax.axis_index("dp")
        chip, core = me // cores, me % cores
        order = [(k, c) for c in range(cores) for k in range(chips)]
        groups = jnp.stack(
            [((chip + chips - k) % chips) * cores + (core + c) % cores for k, c in order]
        ).astype(jnp.int32)

        def from_chip(x, k):
            pairs = [
                (a * cores + c, ((a + k) % chips) * cores + c)
                for a in range(chips)
                for c in range(cores)
            ]
            return lax.ppermute(x, "dp", pairs)

        def from_core(x):
            pairs = [
                (a * cores + c, a * cores + (c + 1) % cores)
                for a in range(chips)
                for c in range(cores)
            ]
            return lax.ppermute(x, "dp", pairs)

        tie = lax.optimization_barrier
        row = lax.axis_index("rows")
        pos = jnp.where(row % 2 == 0, row // 2, n - 1 - row // 2)
        height = moment1.shape[1]

        def start_of(q):
            q = (q + 2 * n) % n
            return jnp.where(q < n // 2, 2 * q, 2 * (n - 1 - q) + 1) * height

        def hop(x, way):
            return lax.ppermute(
                x, "rows", [(ring[q], ring[(q + way) % n]) for q in range(n)]
            )

        def block(partial, q):
            return lax.dynamic_slice_in_dim(partial, start_of(q), height, 0)

        def hops_of(i):
            near, far = (n - 1) // 2, n // 2
            return ((1, far), (-1, near)) if i % 2 == 0 else ((1, near), (-1, far))

        def reduce_pair(held):
            if n > LONGEST_RING:
                return [
                    lax.psum_scatter(p, "rows", scatter_dimension=0, tiled=True)
                    for p in held
                ]
            sums = [block(p, pos) for p in held]
            live = {}
            for i, p in enumerate(held):
                for way, far in hops_of(i):
                    if far:
                        live[i, way] = block(p, pos + way * far)
            for step in range(n // 2):
                for i, p in enumerate(held):
                    for way, far in hops_of(i):
                        if step >= far:
                            continue
                        got = hop(live[i, way], way)
                        if step == far - 1:
                            sums[i] = sums[i] + got
                        else:
                            live[i, way] = got + block(p, pos + way * (far - 1 - step))
            return sums

        def gather_pair(held):
            if n > LONGEST_RING:
                return [lax.all_gather(x, "rows", axis=0, tiled=True) for x in held]
            full = []
            for x in held:
                empty = jnp.zeros((height * n, x.shape[1]), x.dtype)
                full.append(lax.dynamic_update_slice_in_dim(empty, x, row * height, 0))
            live = {(i, way): x for i, x in enumerate(held) for way in (1, -1)}
            for step in range(n // 2):
                for i in range(len(held)):
                    for way, far in hops_of(i):
                        if step >= far:
                            continue
                        live[i, way] = hop(live[i, way], way)
                        full[i] = lax.dynamic_update_slice_in_dim(
                            full[i], live[i, way], start_of(pos - way * (step + 1)), 0
                        )
            return full

        firsts, seconds, exchanged = [], [], []

        def finish(number, pair, sums):
            updates = []
            for (m, s), projected in zip(pair, sums):
                first, second, update = moment_step(
                    projected, part(moment1, m, s), part(moment2, m, s), scale
                )
                firsts.append(first)
                seconds.append(second)
                updates.append(update)
            for (m, s), full in zip(pair, gather_pair(updates)):
                back = jnp.dot(basis[m], full, preferred_element_type=jnp.float32)
                fresh = part(weights, m, s).astype(jnp.float32) - 0.5 * back
                fresh = fresh.astype(jnp.bfloat16)
                exchanged.append([fresh] + [from_chip(fresh, k) for k in range(1, chips)])

        sums = None
        pairs = [chunks[i : i + 2] for i in range(0, len(chunks), 2)]
        for number, pair in enumerate(pairs):
            held = partials[2 * number : 2 * number + 2]
            if sums is not None:
                held, sums = tie((held, sums))
            sums_before, sums = sums, reduce_pair(held)
            if number >= 1:
                finish(number - 1, pairs[number - 1], sums_before)
                sums, exchanged[-2][0], exchanged[-1][0] = tie(
                    (sums, exchanged[-2][0], exchanged[-1][0])
                )
        finish(len(pairs) - 1, pairs[-1], sums)

        shape = (mats, rows, cols * dp)
        count = len(chunks)
        out = None
        for i, (m, s) in enumerate(chunks):
            pieces = list(exchanged[i])
            if i < count - 2:
                pieces[1:], exchanged[-1][0] = tie((pieces[1:], exchanged[-1][0]))
            if i >= 2:
                pieces[1:], out = tie((pieces[1:], out))
            if cores == 2:
                pieces = pieces + [from_core(x) for x in pieces]
            out = place(groups, pieces, out, shape, m, s)

        def whole(parts):
            return jnp.stack(
                [
                    jnp.concatenate(parts[m * SPLITS : (m + 1) * SPLITS], axis=1)
                    for m in range(mats)
                ]
            )

        return (out, whole(firsts), whole(seconds))

    return jax.shard_map(
        local,
        mesh=mesh,
        in_specs=(
            P(None, "rows", "dp"),
            P(None, "rows", None),
            P(None, "rows", "dp"),
            P(None, "rows", "dp"),
            P(None, "rows", "dp"),
        ),
        out_specs=(P(None, "rows", None), P(None, "rows", "dp"), P(None, "rows", "dp")),
        check_vma=False,
    )
```
